32 devices in a mesh: seq: 8 (over z, x), head: 4 (over y, core).
Axes of the slice: x: 2, y: 2, z: 4, core: 2. Of those that a mesh axis runs over, the one named last changes fastest.
Arguments:
- queries: bfloat16 [1024, 3072], P('seq', 'head'), may hold values from -8 to 8
- latents: bfloat16 [1024, 576], P('seq'), may hold values from -8 to 8
- key_up: bfloat16 [512, 2048], P(None, 'head'), may hold values from -0.25 to 0.25
- value_up: bfloat16 [512, 2048], P(None, 'head'), may hold values from -0.25 to 0.25
- out_grad: bfloat16 [1024, 2048], P('seq', 'head'), may hold values from -48 to 48
- positions: int32 [1024], P('seq'), may hold values from 0 to 1023, as said below
Outputs:
- query_grad: bfloat16 [1024, 3072], P('seq', 'head')
- latent_grad: float32 [1024, 576], P('seq')
- key_up_grad: float32 [512, 2048], P(None, 'head')
- value_up_grad: float32 [512, 2048], P(None, 'head')
The draws below stay inside these ranges and needn't reach their ends.
Inputs may be any that keep to these rules, and one draw needn't show every extreme that they name: Every position from 0 to 1023 occurs once; positions come in stripes of 128 consecutive positions in ascending order, each stripe whole within the rows of one device.
All inputs are finite; a program needn't handle non-finite values.
Results may differ from the reference program's by a relative error of at most 0.0084.
Values may be sent and summed in bfloat16 or wider, within the bound.
A program may use at most 64 MiB of HBM per device.

```python
import math
import jax
import jax.numpy as jnp
from jax import lax

D_LAT = 512
D_ROPE = 64
D_NOPE = 128
D_V = 128
STRIPE = 128
HEADS = 16
SEQ = 1024


def stripe_positions(key):
    order = jax.random.permutation(jax.random.fold_in(key, 11), SEQ // STRIPE).astype(jnp.int32)
    within = jnp.arange(STRIPE, dtype=jnp.int32)
    return (order[:, None] * STRIPE + within[None, :]).reshape(SEQ)


def draw_positions(key, part):
    return stripe_positions(key)


def draw_queries(key, part):
    width = HEADS * (D_NOPE + D_ROPE)
    own = jax.random.fold_in(key, 21)
    base = jax.random.normal(own, (SEQ, width), jnp.float32)
    return jnp.clip(base, -8.0, 8.0).astype(jnp.bfloat16)


def draw_latents(key, part):
    width = D_LAT + D_ROPE
    own = jax.random.fold_in(key, 31)
    base = jax.random.normal(own, (SEQ, width), jnp.float32)
    return jnp.clip(base, -8.0, 8.0).astype(jnp.bfloat16)


def block_levels(stream_key, extent, pieces, least, top_value):
    factor_of = 1.0
    for position, shards_of in pieces:
        steps = jax.random.uniform(jax.random.fold_in(jax.random.fold_in(stream_key, 6), position), (shards_of,), jnp.float32, least / len(pieces), top_value / len(pieces))
        factor_of = factor_of * jnp.repeat(jnp.exp(steps), extent[position] // shards_of).reshape((-1,) + (1,) * (len(extent) - 1 - position))
    return factor_of


def normal_values(own_key, dims, deviation, limit, pieces=(), held_as=jnp.bfloat16):
    factor_of = block_levels(own_key, dims, pieces, -0.22, 0.18) if pieces else 1.0
    entries = jax.random.normal(own_key, dims, jnp.float32) * deviation * factor_of
    return jnp.minimum(jnp.maximum(entries, -limit), limit).astype(held_as)


def setup_inputs(seed: int = 0) -> dict:
    key_of = jax.random.split(jax.random.key(seed), 7)
    return {
        "queries": draw_queries(jax.random.fold_in(key_of[6], 71), 0),
        "latents": draw_latents(jax.random.fold_in(key_of[6], 71), 0),
        "key_up": normal_values(key_of[2], (D_LAT, HEADS * D_NOPE), D_LAT ** -0.5, 0.25, ((1, 4),)),
        "value_up": normal_values(key_of[3], (D_LAT, HEADS * D_V), D_LAT ** -0.5, 0.25, ((1, 4),)),
        "out_grad": normal_values(key_of[4], (SEQ, HEADS * D_V), 8.0, 48.0, ((0, 8), (1, 4))),
        "positions": draw_positions(jax.random.fold_in(key_of[6], 71), 0),
    }


NEG = -1e+30

def reference(queries, latents, key_up, value_up, out_grad, positions):
    seq = latents.shape[0]
    heads = key_up.shape[1] // D_NOPE
    qk = D_NOPE + D_ROPE
    scale = 1.0 / math.sqrt(qk)
    compressed = latents[:, :D_LAT]
    rope_keys = latents[:, D_LAT:].astype(jnp.float32)
    key_nope = jnp.dot(compressed, key_up, preferred_element_type=jnp.float32).astype(jnp.bfloat16)
    values = jnp.dot(compressed, value_up, preferred_element_type=jnp.float32).astype(jnp.bfloat16)
    key_heads = lax.optimization_barrier(key_nope).astype(jnp.float32).reshape(seq, heads, D_NOPE)
    value_heads = lax.optimization_barrier(values).astype(jnp.float32).reshape(seq, heads, D_V)
    block = math.gcd(seq, 512)
    nblocks = seq // block
    q_blocks = queries.reshape(nblocks, block, heads, qk)
    g_blocks = out_grad.reshape(nblocks, block, heads, D_V)
    p_blocks = positions.reshape(nblocks, block)

    def one_block(carry, inputs):
        key_acc, rope_acc, value_acc = carry
        q_block, g_block, pos_block = inputs
        q_nope = q_block[:, :, :D_NOPE].astype(jnp.float32)
        q_rope = q_block[:, :, D_NOPE:].astype(jnp.float32)
        grads = g_block.astype(jnp.float32)
        scores = jnp.einsum('bhd,khd->hbk', q_nope, key_heads)
        scores = (scores + jnp.einsum('bhd,kd->hbk', q_rope, rope_keys)) * scale
        visible = (positions[None, :] <= pos_block[:, None])[None]
        masked = jnp.where(visible, scores, NEG)
        top = lax.optimization_barrier(jnp.max(masked, axis=2, keepdims=True))
        total = lax.optimization_barrier(jnp.sum(jnp.exp(jnp.where(visible, scores - top, NEG)), axis=2, keepdims=True))
        lse = top + jnp.log(total)
        probs = jnp.exp(jnp.where(visible, scores - lse, NEG))
        dprobs = jnp.einsum('bhd,khd->hbk', grads, value_heads)
        delta = lax.optimization_barrier(jnp.sum(probs * dprobs, axis=2, keepdims=True))
        dscore16 = (probs * (dprobs - delta) * scale).astype(jnp.bfloat16)
        dscore = lax.optimization_barrier(dscore16).astype(jnp.float32)
        probs16 = lax.optimization_barrier(probs.astype(jnp.bfloat16)).astype(jnp.float32)
        grad_nope = jnp.einsum('hbk,khd->bhd', dscore, key_heads)
        grad_rope = jnp.einsum('hbk,kd->bhd', dscore, rope_keys)
        q_grad = jnp.concatenate([grad_nope, grad_rope], axis=2).reshape(block, heads * qk)
        key_acc = key_acc + jnp.einsum('hbk,bhd->khd', dscore, q_nope)
        rope_acc = rope_acc + jnp.einsum('hbk,bhd->kd', dscore, q_rope)
        value_acc = value_acc + jnp.einsum('hbk,bhd->khd', probs16, grads)
        return ((key_acc, rope_acc, value_acc), q_grad.astype(jnp.bfloat16))
    start = (jnp.zeros((seq, heads, D_NOPE), jnp.float32), jnp.zeros((seq, D_ROPE), jnp.float32), jnp.zeros((seq, heads, D_V), jnp.float32))
    sums, q_grads = lax.scan(one_block, start, (q_blocks, g_blocks, p_blocks))
    key_acc, rope_acc, value_acc = sums
    key_grad = key_acc.reshape(seq, heads * D_NOPE)
    value_grad = value_acc.reshape(seq, heads * D_V)
    high = lax.Precision.HIGHEST
    key_up32 = key_up.astype(jnp.float32)
    value_up32 = value_up.astype(jnp.float32)
    folded = jnp.dot(key_grad, key_up32.T, precision=high)
    folded = folded + jnp.dot(value_grad, value_up32.T, precision=high)
    latent_grad = jnp.concatenate([folded, rope_acc], axis=1)
    compressed32 = compressed.astype(jnp.float32)
    key_up_grad = jnp.dot(compressed32.T, key_grad, precision=high)
    value_up_grad = jnp.dot(compressed32.T, value_grad, precision=high)
    query_grad = q_grads.reshape(seq, heads * qk)
    return (query_grad, latent_grad, key_up_grad, value_up_grad)
```

```python
import itertools
import math

import jax
import jax.numpy as jnp
from jax import lax
from jax.experimental import pallas as pl
from jax.experimental.pallas import tpu as pltpu
from jax.sharding import PartitionSpec as P

D_LAT = 512
D_ROPE = 64
D_NOPE = 128
D_V = 128
D_QK = D_NOPE + D_ROPE
D_ALL = D_LAT + D_ROPE
LANE = 128
STRIPE = 128
NEG = -1e30
LOG2E = 1.4426950408889634
MESH = pl.DeviceIdType.MESH
F32 = jnp.float32
BF16 = jnp.bfloat16


def bit(index, b):
    return (index // (1 << b)) % 2


def flip(index, b):
    return index + (1 << b) * (1 - 2 * bit(index, b))


def xor(index, mask):
    b = 0
    while mask >> b:
        if (mask >> b) & 1:
            index = flip(index, b)
        b += 1
    return index


def pick(index, bits):
    out = 0
    for k, b in enumerate(bits):
        out = out + (1 << k) * bit(index, b)
    return out


def put(index, bits, value):
    for k, b in enumerate(bits):
        index = index + (1 << b) * (((value >> k) & 1) - bit(index, b))
    return index


def nn(a, b):
    return lax.dot_general(a, b, (((1,), (0,)), ((), ())), preferred_element_type=F32)


def nt(a, b):
    return lax.dot_general(a, b, (((1,), (1,)), ((), ())), preferred_element_type=F32)


def loop(n, body, init):
    if n <= 8:
        for t in range(n):
            init = body(t, init)
        return init
    return lax.fori_loop(0, n, body, init)


class Sems:
    def __init__(self, send, recv):
        self.send, self.recv, self.used = send, recv, 0
        self.sent = []

    def copy(self, src, dst, device):
        k = self.used
        self.used += 1
        copy = pltpu.make_async_remote_copy(
            src_ref=src,
            dst_ref=dst,
            send_sem=self.send.at[k],
            recv_sem=self.recv.at[k],
            device_id=device,
            device_id_type=MESH,
        )
        copy.start()
        self.sent.append(copy)
        return copy


def kernel(
    nseq, nhead, subs,
    q_ref, lat_ref, ku_ref, vu_ref, do_ref, pos_ref,
    dq_ref, dl_ref, dk_ref, dv_ref,
    stage, qd, qall, dall, lat, pos, kt, vt, kuv, ut, sc, dp, mx, sinv, sdel,
    pr, ds, kvg, rp, up, ur, fin, lg, rc, ry, rx, ac, rz, fl, dqt, dqr,
    send, recv,
):
    seq, head = lax.axis_index("seq"), lax.axis_index("head")
    rows = lat_ref.shape[1]
    heads = ku_ref.shape[1] // D_NOPE
    nq, nk = heads * rows, nseq * rows
    nb = nseq.bit_length() - 1
    hb = heads.bit_length() - 1
    member_bits = [0] + list(range(nb - hb + 1, nb))
    group_bits = [b for b in range(nb) if b not in member_bits]
    groups = 1 << len(group_bits)
    nz = nseq // 2
    sub = D_ALL // nhead
    scale = 1.0 / math.sqrt(D_QK)
    sems = Sems(send, recv)
    u, w = pick(seq, member_bits), pick(seq, group_bits)
    x, z = bit(seq, 0), seq // 2
    core, y = bit(head, 0), bit(head, 1)

    def on_seq(s):
        return (s, head)

    def on_head(h):
        return (seq, h)

    other = on_head(flip(head, 0))
    across = on_head(flip(head, 1))

    barrier = pltpu.get_barrier_semaphore()
    for mask in range(1, nseq):
        pl.semaphore_signal(barrier, inc=1, device_id=on_seq(xor(seq, mask)), device_id_type=MESH)
    for device in (other, across):
        pl.semaphore_signal(barrier, inc=1, device_id=device, device_id_type=MESH)

    def at(start, size, step):
        return pl.ds(pl.multiple_of(start * step, step), size)

    for h in range(heads):
        stage[h, :D_QK, :] = q_ref[:, h * D_QK : (h + 1) * D_QK].T
        stage[h, D_QK:, :] = do_ref[:, h * D_V : (h + 1) * D_V].T
    lat[:, at(seq, rows, rows)] = lat_ref[...]
    pos[seq] = pos_ref[...]
    qd[:, at(u, rows, rows)] = stage[u]
    kuv[:, :D_NOPE] = ku_ref[:, at(u, D_NOPE, D_NOPE)]
    kuv[:, D_NOPE:] = vu_ref[:, at(u, D_V, D_V)]
    ut[...] = kuv[...].T
    mx[...] = jnp.full(mx.shape, NEG, F32)

    pl.semaphore_wait(barrier, nseq + 1)

    def gather(order, region, own, arrived):
        pending = {}

        def forward(mask):
            last = max([k for k, b in enumerate(order) if (mask >> b) & 1], default=-1)
            piece = region(xor(seq, mask))
            for b in order[last + 1 :]:
                pending[mask | (1 << b)] = sems.copy(
                    own if mask == 0 else piece, piece, on_seq(flip(seq, b))
                )

        forward(0)
        masks = [
            sum(1 << b for b in some)
            for size in range(1, len(order) + 1)
            for some in itertools.combinations(order, size)
        ]
        for mask in masks:
            yield
            pending[mask].wait_recv()
            forward(mask)
            arrived(mask)

    half = D_ALL // 2
    zbits = list(range(nb - 1, 0, -1))
    passes = {}

    def lat_region(s):
        return lat.at[at(core, half, half), at(s, rows, rows)]

    def pass_on(mask):
        piece = lat_region(xor(seq, mask))
        passes[mask] = sems.copy(piece, piece, other)

    lats = gather(zbits + [0], lat_region, lat_ref.at[at(core, half, half)], pass_on)
    next(lats)
    pos_in = [
        sems.copy(pos_ref, pos.at[seq], on_seq(xor(seq, mask))) for mask in range(1, nseq)
    ]
    q_in = []
    for v in range(1, heads):
        mask = sum(((v >> k) & 1) << b for k, b in enumerate(member_bits))
        there = xor(seq, mask)
        q_in.append(
            sems.copy(stage.at[pick(there, member_bits)], qd.at[:, at(u, rows, rows)], on_seq(there))
        )

    def keys_of(s):
        here = at(s, rows, rows)
        both = nn(ut[...], lat[:D_LAT, here]).astype(BF16)
        kt[:D_NOPE, here] = both[:D_NOPE]
        vt[:, here] = both[D_NOPE:]
        kt[D_NOPE:, here] = lat[D_LAT:, here]

    down = lax.broadcasted_iota(jnp.int32, (STRIPE, rows), 0)
    along = lax.broadcasted_iota(jnp.int32, (1, STRIPE), 1)
    per = rows // STRIPE

    def scores_of(s):
        here = at(s, rows, rows)
        keys, vals = kt[:, here], vt[:, here]
        rel = pos[s] - down
        for t in range(nq // STRIPE):
            part = slice(t * STRIPE, (t + 1) * STRIPE)
            cut = (t % per) * STRIPE
            first = pos[put(seq, member_bits, t // per)][:, cut : cut + STRIPE] - along
            first = jnp.concatenate([first] * per, axis=1)
            got = jnp.where(rel <= first, nn(qall[part, :], keys), NEG)
            sc[part, here] = got
            dp[part, here] = nn(dall[part, :], vals)
            top = mx[part, :]
            for c in range(rows // LANE):
                top = jnp.maximum(top, got[:, c * LANE : (c + 1) * LANE])
            mx[part, :] = top

    keys_of(seq)
    for copy in q_in:
        copy.wait_recv()
    qall[...] = qd[:D_QK, :].T
    dall[...] = qd[D_QK:, :].T
    for copy in pos_in:
        copy.wait_recv()
    scores_of(seq)
    order = zbits + [0]
    masks = [
        sum(1 << b for b in some)
        for size in range(1, len(order) + 1)
        for some in itertools.combinations(order, size)
    ]
    ready = []
    for mask in masks:
        next(lats, None)
        ready.append(mask)
        if len(ready) > 2:
            block = ready.pop(0)
            passes[block].wait_recv()
            keys_of(xor(seq, block))
            scores_of(xor(seq, block))
    for block in ready:
        passes[block].wait_recv()
        keys_of(xor(seq, block))
        scores_of(xor(seq, block))

    factor = scale * LOG2E
    for t in range(nq // STRIPE):
        part = slice(t * STRIPE, (t + 1) * STRIPE)
        top = jnp.max(mx[part, :], axis=1, keepdims=True) * factor

        def sums(k, carry):
            total, weighted = carry
            here = at(k, LANE, LANE)
            e = jnp.exp2(sc[part, here] * factor - top)
            sc[part, here] = e
            return total + e, weighted + e * dp[part, here]

        zero = jnp.zeros((STRIPE, LANE), F32)
        total, weighted = loop(nk // LANE, sums, (zero, zero))
        total = jnp.sum(total, axis=1, keepdims=True)
        weighted = jnp.sum(weighted, axis=1, keepdims=True)
        inv = 1.0 / total
        sinv[part, :] = jnp.broadcast_to(inv, (STRIPE, LANE))
        sdel[part, :] = jnp.broadcast_to(weighted * inv, (STRIPE, LANE))

        def norm(k, carry):
            here = at(k, LANE, LANE)
            prob = sc[part, here] * sinv[part, :]
            sc[part, here] = prob
            pr[part, here] = prob.astype(BF16)
            return carry

        loop(nk // LANE, norm, 0)

    tile = math.gcd(nk, 512)

    def values_grad(k, carry):
        here = at(k, tile, tile)
        kvg[D_NOPE:, here] = nn(qd[D_QK:, :], pr[:, here]).astype(BF16)
        return carry

    loop(nk // tile, values_grad, 0)
    up[0] = nt(lat[:D_LAT, :], kvg[D_NOPE:, :]).astype(BF16)

    share = D_LAT // groups
    piece = share // subs

    def up_pipe(a, i, order, out_ref):
        bits = group_bits[::-1]
        slot = 0
        source = lambda g: up.at[a, at(g * subs + i, piece, piece)]
        for k, b in enumerate(bits):
            rest = bits[k + 1 :]
            copies = []
            for values in itertools.product((0, 1), repeat=len(rest)):
                to, mine = flip(seq, b), seq
                for r, value in zip(rest, values):
                    to = to + (1 << r) * (value - bit(to, r))
                    mine = mine + (1 << r) * (value - bit(mine, r))
                copy = sems.copy(
                    source(pick(to, group_bits)), ur.at[a, i, slot], on_seq(flip(seq, b))
                )
                copies.append((copy, slot, pick(mine, group_bits)))
                slot += 1
            yield
            for copy, got, g in copies:
                copy.wait_recv()
                kept = source(g)
                kept[...] = (kept[...].astype(F32) + ur[a, i, got].astype(F32)).astype(BF16)

        def place(s):
            return (
                at(pick(s, group_bits) * subs + i, piece, piece),
                at(pick(s, member_bits), LANE, LANE),
            )

        def arrived(mask):
            r, c = place(xor(seq, mask))
            out_ref[r, c] = fin[a, r, c].astype(F32)

        r, c = place(seq)
        out_ref[r, c] = source(w)[...].astype(F32)

        def region(s):
            r, c = place(s)
            return fin.at[a, r, c]

        yield from gather(order, region, source(w), arrived)

    def start(pipes):
        return [p for p in pipes if next(p, "end") != "end"]

    ag = zbits + [0]
    live = start([up_pipe(0, i, ag, dv_ref) for i in range(subs)])

    for t in range(nq // STRIPE):
        part = slice(t * STRIPE, (t + 1) * STRIPE)

        def scored(k, carry):
            here = at(k, LANE, LANE)
            ds[part, here] = (
                sc[part, here] * (dp[part, here] - sdel[part, :]) * scale
            ).astype(BF16)
            return carry

        loop(nk // LANE, scored, 0)

    def keys_grad(k, carry):
        here = at(k, tile, tile)
        got = nn(qd[:D_QK, :], ds[:, here]).astype(BF16)
        kvg[:D_NOPE, here] = got[:D_NOPE]
        rp[:, here] = got[D_NOPE:]
        return carry

    loop(nk // tile, keys_grad, 0)
    up[1] = nt(lat[:D_LAT, :], kvg[:D_NOPE, :]).astype(BF16)
    live += start([up_pipe(1, i, ag, dk_ref) for i in range(subs)])

    zmasks = list(range(1, nz))[::-1] + [0]
    to_core, to_y, to_x, to_z = {}, {}, {}, {}
    mine, others = y * 2 + core, (1 - y) * 2 + core

    def fold(k):
        here = at(xor(z, k), 2 * rows, 2 * rows)
        got = nn(kuv[...], kvg[:, here]).astype(BF16)
        got = jnp.concatenate([got, rp[:, here]], axis=0)
        for h in range(nhead):
            lg[h, k] = got[h * sub : (h + 1) * sub]
        to_core[k] = [
            sems.copy(lg.at[t * 2 + 1 - core, k], rc.at[j, k], other)
            for j, t in ((0, 1 - y), (1, y))
        ]

    def add_core(k):
        to_core[k][0].wait_recv()
        lg[others, k] = (lg[others, k].astype(F32) + rc[0, k].astype(F32)).astype(BF16)
        to_y[k] = sems.copy(lg.at[others, k], ry.at[k], across)
        to_core[k][1].wait_recv()
        lg[mine, k] = (lg[mine, k].astype(F32) + rc[1, k].astype(F32)).astype(BF16)

    def add_y(k):
        to_y[k].wait_recv()
        lg[mine, k] = (lg[mine, k].astype(F32) + ry[k].astype(F32)).astype(BF16)
        to_x[k] = sems.copy(
            lg.at[mine, k, :, at(1 - x, rows, rows)], rx.at[k], on_seq(flip(seq, 0))
        )

    def add_x(k):
        to_x[k].wait_recv()
        kept = lg[mine, k, :, at(x, rows, rows)].astype(F32) + rx[k].astype(F32)
        ac[k] = kept.astype(BF16)
        if k:
            to_z[k] = sems.copy(ac.at[k], rz.at[k], on_seq(xor(seq, 2 * k)))

    def lat_pipe():
        for stage_of in (add_core, add_y, add_x):
            for k in zmasks:
                stage_of(k)
                yield
        total = ac[0].astype(F32)
        for k in zmasks[:-1]:
            to_z[k].wait_recv()
            total = total + rz[k].astype(F32)
        fl[head] = total.astype(BF16)
        first = sems.copy(fl.at[head], fl.at[head], across)
        second = sems.copy(fl.at[head], fl.at[head], other)
        yield
        first.wait_recv()
        third = sems.copy(fl.at[others], fl.at[others], other)
        second.wait_recv()
        yield
        third.wait_recv()
        for h in range(nhead):
            dl_ref[h * sub : (h + 1) * sub, :] = fl[h].astype(F32)

    for k in zmasks:
        fold(k)
    live = start(live)
    dqt[...] = nt(kt[...], ds[...]).astype(BF16)
    dq_in = []
    for v in range(1, heads):
        mask = sum(((v >> k) & 1) << b for k, b in enumerate(member_bits))
        there = xor(seq, mask)
        dq_in.append(
            sems.copy(
                dqt.at[:, at(pick(there, member_bits), rows, rows)], dqr.at[u], on_seq(there)
            )
        )
    dqr[u] = dqt[:, at(u, rows, rows)]
    live = start(live + [lat_pipe()])

    def dq_pipe():
        for _ in range(6):
            yield
        for copy in dq_in:
            copy.wait_recv()
        for h in range(heads):
            dq_ref[:, h * D_QK : (h + 1) * D_QK] = dqr[h].T

    live += start([dq_pipe()])
    while live:
        live = start(live)
    for copy in sems.sent:
        copy.wait_send()


def make_shards(nseq, nhead):
    def shards(queries, latents, key_up, value_up, out_grad, positions):
        rows, heads = latents.shape[0], key_up.shape[1] // D_NOPE
        nq, nk = heads * rows, nseq * rows
        nz, groups = nseq // 2, nseq // heads
        subs = 2
        share = D_LAT // groups
        sub = D_ALL // nhead
        cols = key_up.shape[1]
        copies = (nseq - 1) * 3 + 2 * (heads - 1)
        copies += 2 * subs * (groups - 1 + nseq - 1) + 5 * nz + 3
        vmem = pl.BlockSpec(memory_space=pltpu.VMEM)
        body = lambda *refs: kernel(nseq, nhead, subs, *refs)
        scratch = [
            ((heads, D_QK + D_V, rows), BF16),
            ((D_QK + D_V, nq), BF16),
            ((nq, D_QK), BF16),
            ((nq, D_V), BF16),
            ((D_ALL, nk), BF16),
            ((nseq, 1, rows), jnp.int32),
            ((D_QK, nk), BF16),
            ((D_V, nk), BF16),
            ((D_LAT, D_NOPE + D_V), BF16),
            ((D_NOPE + D_V, D_LAT), BF16),
            ((nq, nk), F32),
            ((nq, nk), F32),
            ((nq, LANE), F32),
            ((nq, LANE), F32),
            ((nq, LANE), F32),
            ((nq, nk), BF16),
            ((nq, nk), BF16),
            ((D_NOPE + D_V, nk), BF16),
            ((D_ROPE, nk), BF16),
            ((2, D_LAT, LANE), BF16),
            ((2, subs, max(groups - 1, 1), share // subs, LANE), BF16),
            ((2, D_LAT, cols), BF16),
            ((nhead, nz, sub, 2 * rows), BF16),
            ((nhead // 2, nz, sub, 2 * rows), BF16),
            ((nz, sub, 2 * rows), BF16),
            ((nz, sub, rows), BF16),
            ((nz, sub, rows), BF16),
            ((nz, sub, rows), BF16),
            ((nhead, sub, rows), BF16),
            ((D_QK, nq), BF16),
            ((heads, D_QK, rows), BF16),
        ]
        limit = 8 * 1024 * 1024
        for shape, dtype in scratch:
            padded = (-(-shape[-1] // LANE) * LANE) * (-(-shape[-2] // 16) * 16)
            limit += math.prod(shape[:-2]) * padded * jnp.dtype(dtype).itemsize
        dq, dl, dk, dv = pl.pallas_call(
            body,
            out_shape=(
                jax.ShapeDtypeStruct(queries.shape, BF16),
                jax.ShapeDtypeStruct((D_ALL, rows), F32),
                jax.ShapeDtypeStruct(key_up.shape, F32),
                jax.ShapeDtypeStruct(value_up.shape, F32),
            ),
            in_specs=[vmem] * 6,
            out_specs=(vmem,) * 4,
            scratch_shapes=[pltpu.VMEM(shape, dtype) for shape, dtype in scratch]
            + [pltpu.SemaphoreType.DMA((copies,)), pltpu.SemaphoreType.DMA((copies,))],
            compiler_params=pltpu.CompilerParams(
                collective_id=0, has_side_effects=True, vmem_limit_bytes=min(limit, 60 * 1024 * 1024)
            ),
        )(queries, latents.T, key_up, value_up, out_grad, positions[None, :])
        return dq, dl.T, dk, dv

    return shards


def solution(mesh):
    in_specs = (
        P("seq", "head"),
        P("seq", None),
        P(None, "head"),
        P(None, "head"),
        P("seq", "head"),
        P("seq"),
    )
    out_specs = (P("seq", "head"), P("seq", None), P(None, "head"), P(None, "head"))
    shards = make_shards(mesh.shape["seq"], mesh.shape["head"])
    return jax.shard_map(shards, mesh=mesh, in_specs=in_specs, out_specs=out_specs, check_vma=False)
```

```python
import itertools
import math

import jax
import jax.numpy as jnp
from jax import lax
from jax.experimental import pallas as pl
from jax.experimental.pallas import tpu as pltpu
from jax.sharding import PartitionSpec as P

D_LAT = 512
D_ROPE = 64
D_NOPE = 128
D_V = 128
D_QK = D_NOPE + D_ROPE
D_ALL = D_LAT + D_ROPE
LANE = 128
STRIPE = 128
NEG = -1e30
LOG2E = 1.4426950408889634
MESH = pl.DeviceIdType.MESH
F32 = jnp.float32
BF16 = jnp.bfloat16


def bit(index, b):
    return (index // (1 << b)) % 2


def flip(index, b):
    return index + (1 << b) * (1 - 2 * bit(index, b))


def xor(index, mask):
    b = 0
    while mask >> b:
        if (mask >> b) & 1:
            index = flip(index, b)
        b += 1
    return index


def pick(index, bits):
    out = 0
    for k, b in enumerate(bits):
        out = out + (1 << k) * bit(index, b)
    return out


def put(index, bits, value):
    for k, b in enumerate(bits):
        index = index + (1 << b) * (((value >> k) & 1) - bit(index, b))
    return index


def nn(a, b):
    return lax.dot_general(a, b, (((1,), (0,)), ((), ())), preferred_element_type=F32)


def nt(a, b):
    return lax.dot_general(a, b, (((1,), (1,)), ((), ())), preferred_element_type=F32)


def loop(n, body, init):
    if n <= 8:
        for t in range(n):
            init = body(t, init)
        return init
    return lax.fori_loop(0, n, body, init)


class Sems:
    def __init__(self, send, recv):
        self.send, self.recv, self.used = send, recv, 0
        self.sent = []

    def copy(self, src, dst, device):
        k = self.used
        self.used += 1
        copy = pltpu.make_async_remote_copy(
            src_ref=src,
            dst_ref=dst,
            send_sem=self.send.at[k],
            recv_sem=self.recv.at[k],
            device_id=device,
            device_id_type=MESH,
        )
        copy.start()
        self.sent.append(copy)
        return copy


def kernel(
    nseq, nhead, subs,
    q_in, lat_in, ku_in, vu_in, do_in, pos_in,
    dq_ref, dl_ref, dk_ref, dv_ref,
    q_ref, lat_ref, do_ref, pos_ref, load,
    stage, qd, qall, dall, lat, pos, kt, vt, kuv, ut, sc, dp, mx, sinv, sdel,
    pr, ds, kvg, rp, up, ur, fin, lg, rc, ry, rx, ac, rz, fl, dqt, dqr,
    send, recv,
):
    seq, head = lax.axis_index("seq"), lax.axis_index("head")
    rows = lat_in.shape[1]
    heads = ku_in.shape[1] // D_NOPE
    nq, nk = heads * rows, nseq * rows
    nb = nseq.bit_length() - 1
    hb = heads.bit_length() - 1
    member_bits = [0] + list(range(nb - hb + 1, nb))
    group_bits = [b for b in range(nb) if b not in member_bits]
    groups = 1 << len(group_bits)
    nz = nseq // 2
    sub = D_ALL // nhead
    scale = 1.0 / math.sqrt(D_QK)
    sems = Sems(send, recv)
    u, w = pick(seq, member_bits), pick(seq, group_bits)
    x, z = bit(seq, 0), seq // 2
    core, y = bit(head, 0), bit(head, 1)

    def on_seq(s):
        return (s, head)

    def on_head(h):
        return (seq, h)

    other = on_head(flip(head, 0))
    across = on_head(flip(head, 1))

    barrier = pltpu.get_barrier_semaphore()
    for mask in range(1, nseq):
        pl.semaphore_signal(barrier, inc=1, device_id=on_seq(xor(seq, mask)), device_id_type=MESH)
    for device in (other, across):
        pl.semaphore_signal(barrier, inc=1, device_id=device, device_id_type=MESH)

    def at(start, size, step):
        return pl.ds(pl.multiple_of(start * step, step), size)

    mine_k, mine_v = at(u, D_NOPE, D_NOPE), at(u, D_V, D_V)
    loads = [
        pltpu.make_async_copy(src, dst, load.at[k])
        for k, (src, dst) in enumerate((
            (lat_in, lat_ref),
            (q_in, q_ref),
            (do_in, do_ref),
            (pos_in, pos_ref),
            (ku_in.at[:, mine_k], kuv.at[:, :D_NOPE]),
            (vu_in.at[:, mine_v], kuv.at[:, D_NOPE:]),
        ))
    ]
    for copy in loads:
        copy.start()
    mx[...] = jnp.full(mx.shape, NEG, F32)
    for copy in loads:
        copy.wait()
    for h in range(heads):
        stage[h, :D_QK, :] = q_ref[:, h * D_QK : (h + 1) * D_QK].T
        stage[h, D_QK:, :] = do_ref[:, h * D_V : (h + 1) * D_V].T
    lat[:, at(seq, rows, rows)] = lat_ref[...]
    pos[seq] = pos_ref[...]
    qd[:, at(u, rows, rows)] = stage[u]
    ut[...] = kuv[...].T

    pl.semaphore_wait(barrier, nseq + 1)

    def gather(order, region, own, arrived):
        pending = {}

        def forward(mask):
            last = max([k for k, b in enumerate(order) if (mask >> b) & 1], default=-1)
            piece = region(xor(seq, mask))
            for b in order[last + 1 :]:
                pending[mask | (1 << b)] = sems.copy(
                    own if mask == 0 else piece, piece, on_seq(flip(seq, b))
                )

        forward(0)
        masks = [
            sum(1 << b for b in some)
            for size in range(1, len(order) + 1)
            for some in itertools.combinations(order, size)
        ]
        for mask in masks:
            yield
            pending[mask].wait_recv()
            forward(mask)
            arrived(mask)

    half = D_ALL // 2
    zbits = list(range(nb - 1, 0, -1))
    passes = {}

    def lat_region(s):
        return lat.at[at(core, half, half), at(s, rows, rows)]

    def pass_on(mask):
        piece = lat_region(xor(seq, mask))
        passes[mask] = sems.copy(piece, piece, other)

    lats = gather(zbits + [0], lat_region, lat_ref.at[at(core, half, half)], pass_on)
    next(lats)
    pos_got = [
        sems.copy(pos_ref, pos.at[seq], on_seq(xor(seq, mask))) for mask in range(1, nseq)
    ]
    q_got = []
    for v in range(1, heads):
        mask = sum(((v >> k) & 1) << b for k, b in enumerate(member_bits))
        there = xor(seq, mask)
        q_got.append(
            sems.copy(stage.at[pick(there, member_bits)], qd.at[:, at(u, rows, rows)], on_seq(there))
        )

    def keys_of(s):
        here = at(s, rows, rows)
        both = nn(ut[...], lat[:D_LAT, here]).astype(BF16)
        kt[:D_NOPE, here] = both[:D_NOPE]
        vt[:, here] = both[D_NOPE:]
        kt[D_NOPE:, here] = lat[D_LAT:, here]

    down = lax.broadcasted_iota(jnp.int32, (STRIPE, rows), 0)
    along = lax.broadcasted_iota(jnp.int32, (1, STRIPE), 1)
    per = rows // STRIPE

    def scores_of(s):
        here = at(s, rows, rows)
        keys, vals = kt[:, here], vt[:, here]
        rel = pos[s] - down
        for t in range(nq // STRIPE):
            part = slice(t * STRIPE, (t + 1) * STRIPE)
            cut = (t % per) * STRIPE
            first = pos[put(seq, member_bits, t // per)][:, cut : cut + STRIPE] - along
            first = jnp.concatenate([first] * per, axis=1)
            got = jnp.where(rel <= first, nn(qall[part, :], keys), NEG)
            sc[part, here] = got
            dp[part, here] = nn(dall[part, :], vals)
            top = mx[part, :]
            for c in range(rows // LANE):
                top = jnp.maximum(top, got[:, c * LANE : (c + 1) * LANE])
            mx[part, :] = top

    keys_of(seq)
    for copy in q_got:
        copy.wait_recv()
    qall[...] = qd[:D_QK, :].T
    dall[...] = qd[D_QK:, :].T
    for copy in pos_got:
        copy.wait_recv()
    scores_of(seq)
    order = zbits + [0]
    masks = [
        sum(1 << b for b in some)
        for size in range(1, len(order) + 1)
        for some in itertools.combinations(order, size)
    ]
    ready = []
    for mask in masks:
        next(lats, None)
        ready.append(mask)
        if len(ready) > 2:
            block = ready.pop(0)
            passes[block].wait_recv()
            keys_of(xor(seq, block))
            scores_of(xor(seq, block))
    for block in ready:
        passes[block].wait_recv()
        keys_of(xor(seq, block))
        scores_of(xor(seq, block))

    factor = scale * LOG2E
    for t in range(nq // STRIPE):
        part = slice(t * STRIPE, (t + 1) * STRIPE)
        top = jnp.max(mx[part, :], axis=1, keepdims=True) * factor

        def sums(k, carry):
            total, weighted = carry
            here = at(k, LANE, LANE)
            e = jnp.exp2(sc[part, here] * factor - top)
            sc[part, here] = e
            return total + e, weighted + e * dp[part, here]

        zero = jnp.zeros((STRIPE, LANE), F32)
        total, weighted = loop(nk // LANE, sums, (zero, zero))
        total = jnp.sum(total, axis=1, keepdims=True)
        weighted = jnp.sum(weighted, axis=1, keepdims=True)
        inv = 1.0 / total
        sinv[part, :] = jnp.broadcast_to(inv, (STRIPE, LANE))
        sdel[part, :] = jnp.broadcast_to(weighted * inv, (STRIPE, LANE))

        def norm(k, carry):
            here = at(k, LANE, LANE)
            prob = sc[part, here] * sinv[part, :]
            sc[part, here] = prob
            pr[part, here] = prob.astype(BF16)
            return carry

        loop(nk // LANE, norm, 0)

    tile = math.gcd(nk, 512)

    def values_grad(k, carry):
        here = at(k, tile, tile)
        kvg[D_NOPE:, here] = nn(qd[D_QK:, :], pr[:, here]).astype(BF16)
        return carry

    loop(nk // tile, values_grad, 0)
    up[0] = nt(lat[:D_LAT, :], kvg[D_NOPE:, :]).astype(BF16)

    share = D_LAT // groups
    piece = share // subs

    def up_pipe(a, i, order, out_ref):
        bits = group_bits[::-1]
        slot = 0
        source = lambda g: up.at[a, at(g * subs + i, piece, piece)]
        for k, b in enumerate(bits):
            rest = bits[k + 1 :]
            copies = []
            for values in itertools.product((0, 1), repeat=len(rest)):
                to, mine = flip(seq, b), seq
                for r, value in zip(rest, values):
                    to = to + (1 << r) * (value - bit(to, r))
                    mine = mine + (1 << r) * (value - bit(mine, r))
                copy = sems.copy(
                    source(pick(to, group_bits)), ur.at[a, i, slot], on_seq(flip(seq, b))
                )
                copies.append((copy, slot, pick(mine, group_bits)))
                slot += 1
            yield
            for copy, got, g in copies:
                copy.wait_recv()
                kept = source(g)
                kept[...] = (kept[...].astype(F32) + ur[a, i, got].astype(F32)).astype(BF16)

        def place(s):
            return (
                at(pick(s, group_bits) * subs + i, piece, piece),
                at(pick(s, member_bits), LANE, LANE),
            )

        def arrived(mask):
            r, c = place(xor(seq, mask))
            out_ref[r, c] = fin[a, r, c].astype(F32)

        r, c = place(seq)
        out_ref[r, c] = source(w)[...].astype(F32)

        def region(s):
            r, c = place(s)
            return fin.at[a, r, c]

        yield from gather(order, region, source(w), arrived)

    def start(pipes):
        return [p for p in pipes if next(p, "end") != "end"]

    ag = zbits + [0]
    live = start([up_pipe(0, i, ag, dv_ref) for i in range(subs)])

    for t in range(nq // STRIPE):
        part = slice(t * STRIPE, (t + 1) * STRIPE)

        def scored(k, carry):
            here = at(k, LANE, LANE)
            ds[part, here] = (
                sc[part, here] * (dp[part, here] - sdel[part, :]) * scale
            ).astype(BF16)
            return carry

        loop(nk // LANE, scored, 0)

    def keys_grad(k, carry):
        here = at(k, tile, tile)
        got = nn(qd[:D_QK, :], ds[:, here]).astype(BF16)
        kvg[:D_NOPE, here] = got[:D_NOPE]
        rp[:, here] = got[D_NOPE:]
        return carry

    loop(nk // tile, keys_grad, 0)
    up[1] = nt(lat[:D_LAT, :], kvg[:D_NOPE, :]).astype(BF16)
    live += start([up_pipe(1, i, ag, dk_ref) for i in range(subs)])

    zmasks = list(range(1, nz))[::-1] + [0]
    to_core, to_y, to_x, to_z = {}, {}, {}, {}
    mine, others = y * 2 + core, (1 - y) * 2 + core

    def fold(k):
        here = at(xor(z, k), 2 * rows, 2 * rows)
        got = nn(kuv[...], kvg[:, here]).astype(BF16)
        got = jnp.concatenate([got, rp[:, here]], axis=0)
        for h in range(nhead):
            lg[h, k] = got[h * sub : (h + 1) * sub]
        to_core[k] = [
            sems.copy(lg.at[t * 2 + 1 - core, k], rc.at[j, k], other)
            for j, t in ((0, 1 - y), (1, y))
        ]

    def add_core(k):
        to_core[k][0].wait_recv()
        lg[others, k] = (lg[others, k].astype(F32) + rc[0, k].astype(F32)).astype(BF16)
        to_y[k] = sems.copy(lg.at[others, k], ry.at[k], across)
        to_core[k][1].wait_recv()
        lg[mine, k] = (lg[mine, k].astype(F32) + rc[1, k].astype(F32)).astype(BF16)

    def add_y(k):
        to_y[k].wait_recv()
        lg[mine, k] = (lg[mine, k].astype(F32) + ry[k].astype(F32)).astype(BF16)
        to_x[k] = sems.copy(
            lg.at[mine, k, :, at(1 - x, rows, rows)], rx.at[k], on_seq(flip(seq, 0))
        )

    def add_x(k):
        to_x[k].wait_recv()
        kept = lg[mine, k, :, at(x, rows, rows)].astype(F32) + rx[k].astype(F32)
        ac[k] = kept.astype(BF16)
        if k:
            to_z[k] = sems.copy(ac.at[k], rz.at[k], on_seq(xor(seq, 2 * k)))

    def lat_pipe():
        for stage_of in (add_core, add_y, add_x):
            for k in zmasks:
                stage_of(k)
                yield
        total = ac[0].astype(F32)
        for k in zmasks[:-1]:
            to_z[k].wait_recv()
            total = total + rz[k].astype(F32)
        fl[head] = total.astype(BF16)
        first = sems.copy(fl.at[head], fl.at[head], across)
        second = sems.copy(fl.at[head], fl.at[head], other)
        yield
        first.wait_recv()
        third = sems.copy(fl.at[others], fl.at[others], other)
        second.wait_recv()
        yield
        third.wait_recv()
        for h in range(nhead):
            dl_ref[h * sub : (h + 1) * sub, :] = fl[h].astype(F32)

    for k in zmasks:
        fold(k)
    live = start(live)
    dqt[...] = nt(kt[...], ds[...]).astype(BF16)
    dq_in = []
    for v in range(1, heads):
        mask = sum(((v >> k) & 1) << b for k, b in enumerate(member_bits))
        there = xor(seq, mask)
        dq_in.append(
            sems.copy(
                dqt.at[:, at(pick(there, member_bits), rows, rows)], dqr.at[u], on_seq(there)
            )
        )
    dqr[u] = dqt[:, at(u, rows, rows)]
    live = start(live + [lat_pipe()])

    def dq_pipe():
        for _ in range(6):
            yield
        for copy in dq_in:
            copy.wait_recv()
        for h in range(heads):
            dq_ref[:, h * D_QK : (h + 1) * D_QK] = dqr[h].T

    live += start([dq_pipe()])
    while live:
        live = start(live)
    for copy in sems.sent:
        copy.wait_send()


def store(*refs):
    sems = refs[8]
    copies = [pltpu.make_async_copy(refs[k], refs[4 + k], sems.at[k]) for k in range(4)]
    for copy in copies:
        copy.start()
    for copy in copies:
        copy.wait()


def make_shards(nseq, nhead):
    def shards(queries, latents, key_up, value_up, out_grad, positions):
        rows, heads = latents.shape[0], key_up.shape[1] // D_NOPE
        nq, nk = heads * rows, nseq * rows
        nz, groups = nseq // 2, nseq // heads
        subs = 2
        share = D_LAT // groups
        sub = D_ALL // nhead
        cols = key_up.shape[1]
        copies = (nseq - 1) * 3 + 2 * (heads - 1)
        copies += 2 * subs * (groups - 1 + nseq - 1) + 5 * nz + 3
        vmem = pl.BlockSpec(memory_space=pltpu.VMEM)
        body = lambda *refs: kernel(nseq, nhead, subs, *refs)
        moved = [
            (queries.shape, BF16),
            ((D_ALL, rows), BF16),
            (out_grad.shape, BF16),
            ((1, rows), jnp.int32),
        ]
        scratch = [
            ((heads, D_QK + D_V, rows), BF16),
            ((D_QK + D_V, nq), BF16),
            ((nq, D_QK), BF16),
            ((nq, D_V), BF16),
            ((D_ALL, nk), BF16),
            ((nseq, 1, rows), jnp.int32),
            ((D_QK, nk), BF16),
            ((D_V, nk), BF16),
            ((D_LAT, D_NOPE + D_V), BF16),
            ((D_NOPE + D_V, D_LAT), BF16),
            ((nq, nk), F32),
            ((nq, nk), F32),
            ((nq, LANE), F32),
            ((nq, LANE), F32),
            ((nq, LANE), F32),
            ((nq, nk), BF16),
            ((nq, nk), BF16),
            ((D_NOPE + D_V, nk), BF16),
            ((D_ROPE, nk), BF16),
            ((2, D_LAT, LANE), BF16),
            ((2, subs, max(groups - 1, 1), share // subs, LANE), BF16),
            ((2, D_LAT, cols), BF16),
            ((nhead, nz, sub, 2 * rows), BF16),
            ((nhead // 2, nz, sub, 2 * rows), BF16),
            ((nz, sub, 2 * rows), BF16),
            ((nz, sub, rows), BF16),
            ((nz, sub, rows), BF16),
            ((nz, sub, rows), BF16),
            ((nhead, sub, rows), BF16),
            ((D_QK, nq), BF16),
            ((heads, D_QK, rows), BF16),
        ]
        limit = 8 * 1024 * 1024
        for shape, dtype in moved + scratch:
            padded = (-(-shape[-1] // LANE) * LANE) * (-(-shape[-2] // 16) * 16)
            limit += math.prod(shape[:-2]) * padded * jnp.dtype(dtype).itemsize
        dq, dl, dk, dv = pl.pallas_call(
            body,
            out_shape=(
                jax.ShapeDtypeStruct(queries.shape, BF16),
                jax.ShapeDtypeStruct((D_ALL, rows), F32),
                jax.ShapeDtypeStruct(key_up.shape, F32),
                jax.ShapeDtypeStruct(value_up.shape, F32),
            ),
            in_specs=[pl.BlockSpec(memory_space=pltpu.HBM)] * 6,
            out_specs=(vmem,) * 4,
            scratch_shapes=[pltpu.VMEM(shape, dtype) for shape, dtype in moved]
            + [pltpu.SemaphoreType.DMA((6,))]
            + [pltpu.VMEM(shape, dtype) for shape, dtype in scratch]
            + [pltpu.SemaphoreType.DMA((copies,)), pltpu.SemaphoreType.DMA((copies,))],
            compiler_params=pltpu.CompilerParams(
                collective_id=0, has_side_effects=True, vmem_limit_bytes=min(limit, 60 * 1024 * 1024)
            ),
        )(*[
            pltpu.with_memory_space_constraint(a, pltpu.HBM)
            for a in (queries, latents.T, key_up, value_up, out_grad, positions[None, :])
        ])
        done = (dq, dl, dk, dv)
        dq, dl, dk, dv = pl.pallas_call(
            store,
            out_shape=[jax.ShapeDtypeStruct(a.shape, a.dtype) for a in done],
            in_specs=[vmem] * 4,
            out_specs=[pl.BlockSpec(memory_space=pltpu.HBM)] * 4,
            scratch_shapes=[pltpu.SemaphoreType.DMA((4,))],
            compiler_params=pltpu.CompilerParams(vmem_limit_bytes=1024 * 1024),
        )(*done)
        return dq, dl.T, dk, dv

    return shards


def solution(mesh):
    in_specs = (
        P("seq", "head"),
        P("seq", None),
        P(None, "head"),
        P(None, "head"),
        P("seq", "head"),
        P("seq"),
    )
    out_specs = (P("seq", "head"), P("seq", None), P(None, "head"), P(None, "head"))
    shards = make_shards(mesh.shape["seq"], mesh.shape["head"])
    return jax.shard_map(shards, mesh=mesh, in_specs=in_specs, out_specs=out_specs, check_vma=False)
```

```python
import itertools
import math

import jax
import jax.numpy as jnp
from jax import lax
from jax.experimental import pallas as pl
from jax.experimental.pallas import tpu as pltpu
from jax.sharding import PartitionSpec as P

D_LAT = 512
D_ROPE = 64
D_NOPE = 128
D_V = 128
D_QK = D_NOPE + D_ROPE
D_ALL = D_LAT + D_ROPE
LANE = 128
STRIPE = 128
NEG = -1e30
LOG2E = 1.4426950408889634
MESH = pl.DeviceIdType.MESH
F32 = jnp.float32
BF16 = jnp.bfloat16


def bit(index, b):
    return (index // (1 << b)) % 2


def flip(index, b):
    return index + (1 << b) * (1 - 2 * bit(index, b))


def xor(index, mask):
    b = 0
    while mask >> b:
        if (mask >> b) & 1:
            index = flip(index, b)
        b += 1
    return index


def pick(index, bits):
    out = 0
    for k, b in enumerate(bits):
        out = out + (1 << k) * bit(index, b)
    return out


def put(index, bits, value):
    for k, b in enumerate(bits):
        index = index + (1 << b) * (((value >> k) & 1) - bit(index, b))
    return index


def nn(a, b):
    return lax.dot_general(a, b, (((1,), (0,)), ((), ())), preferred_element_type=F32)


def nt(a, b):
    return lax.dot_general(a, b, (((1,), (1,)), ((), ())), preferred_element_type=F32)


def loop(n, body, init):
    if n <= 8:
        for t in range(n):
            init = body(t, init)
        return init
    return lax.fori_loop(0, n, body, init)


class Sems:
    def __init__(self, send, recv):
        self.send, self.recv, self.used = send, recv, 0
        self.sent = []

    def copy(self, src, dst, device):
        k = self.used
        self.used += 1
        copy = pltpu.make_async_remote_copy(
            src_ref=src,
            dst_ref=dst,
            send_sem=self.send.at[k],
            recv_sem=self.recv.at[k],
            device_id=device,
            device_id_type=MESH,
        )
        copy.start()
        self.sent.append(copy)
        return copy


def kernel(
    nseq, nhead, subs,
    q_in, lat_in, ku_in, vu_in, do_in, pos_in,
    dq_ref, dl_ref, dk_ref, dv_ref,
    q_ref, lat_ref, do_ref, pos_ref, load,
    stage, qd, qall, dall, lat, pos, kt, vt, kuv, ut, sc, dp, mx, sinv, sdel,
    pr, ds, kvg, rp, up, ur, fin, lg, rc, ry, rx, ac, rz, fl, dqt, dqr,
    send, recv,
):
    seq, head = lax.axis_index("seq"), lax.axis_index("head")
    rows = lat_in.shape[1]
    heads = ku_in.shape[1] // D_NOPE
    nq, nk = heads * rows, nseq * rows
    nb = nseq.bit_length() - 1
    hb = heads.bit_length() - 1
    member_bits = [0] + list(range(nb - hb + 1, nb))
    group_bits = [b for b in range(nb) if b not in member_bits]
    groups = 1 << len(group_bits)
    nz = nseq // 2
    scale = 1.0 / math.sqrt(D_QK)
    sems = Sems(send, recv)
    u, w = pick(seq, member_bits), pick(seq, group_bits)
    x, z = bit(seq, 0), seq // 2
    core, y = bit(head, 0), bit(head, 1)

    def on_seq(s):
        return (s, head)

    def on_head(h):
        return (seq, h)

    other = on_head(flip(head, 0))
    across = on_head(flip(head, 1))

    barrier = pltpu.get_barrier_semaphore()
    for mask in range(1, nseq):
        pl.semaphore_signal(barrier, inc=1, device_id=on_seq(xor(seq, mask)), device_id_type=MESH)
    for device in (other, across):
        pl.semaphore_signal(barrier, inc=1, device_id=device, device_id_type=MESH)

    def at(start, size, step):
        return pl.ds(pl.multiple_of(start * step, step), size)

    mine_k, mine_v = at(u, D_NOPE, D_NOPE), at(u, D_V, D_V)
    loads = [
        pltpu.make_async_copy(src, dst, load.at[k])
        for k, (src, dst) in enumerate((
            (lat_in, lat_ref),
            (q_in, q_ref),
            (do_in, do_ref),
            (pos_in, pos_ref),
            (ku_in.at[:, mine_k], kuv.at[:, :D_NOPE]),
            (vu_in.at[:, mine_v], kuv.at[:, D_NOPE:]),
        ))
    ]
    for copy in loads:
        copy.start()
    mx[...] = jnp.full(mx.shape, NEG, F32)

    zbits = list(range(nb - 1, 0, -1))
    order = zbits + [0]
    masks = [
        sum(1 << b for b in some)
        for size in range(1, nb + 1)
        for some in itertools.combinations(order, size)
    ]
    levels = [[m for m in masks if m.bit_count() == size] for size in range(1, nb + 1)]
    by_seq, by_core, by_y, by_both = {}, {}, {}, {}
    sub = D_ALL // nhead

    def quarter(h, s):
        return lat.at[at(h, sub, sub), at(s, rows, rows)]

    def forward(mask):
        last = max([k for k, b in enumerate(order) if (mask >> b) & 1], default=-1)
        piece = quarter(head, xor(seq, mask))
        for b in order[last + 1 :]:
            source = piece if mask else lat_ref.at[at(head, sub, sub)]
            by_seq[mask | (1 << b)] = sems.copy(source, piece, on_seq(flip(seq, b)))

    def relay(mask):
        by_seq[mask].wait_recv()
        forward(mask)
        piece = quarter(head, xor(seq, mask))
        by_y[mask] = sems.copy(piece, piece, across)
        by_core[mask] = sems.copy(piece, piece, other)

    def relay_y(mask):
        by_y[mask].wait_recv()
        piece = quarter(flip(head, 1), xor(seq, mask))
        by_both[mask] = sems.copy(piece, piece, other)

    loads[0].wait()
    pl.semaphore_wait(barrier, nseq + 1)
    forward(0)
    for copy in loads[1:4]:
        copy.wait()
    for h in range(heads):
        stage[h, :D_QK, :] = q_ref[:, h * D_QK : (h + 1) * D_QK].T
        stage[h, D_QK:, :] = do_ref[:, h * D_V : (h + 1) * D_V].T
    q_got = []
    for v in range(1, heads):
        mask = sum(((v >> k) & 1) << b for k, b in enumerate(member_bits))
        there = xor(seq, mask)
        q_got.append(
            sems.copy(stage.at[pick(there, member_bits)], qd.at[:, at(u, rows, rows)], on_seq(there))
        )
    pos_got = [
        sems.copy(pos_ref, pos.at[seq], on_seq(xor(seq, mask))) for mask in range(1, nseq)
    ]
    for copy in loads[4:]:
        copy.wait()
    lat[:, at(seq, rows, rows)] = lat_ref[...]
    pos[seq] = pos_ref[...]
    qd[:, at(u, rows, rows)] = stage[u]
    ut[...] = kuv[...].T

    def keys_of(s):
        here = at(s, rows, rows)
        both = nn(ut[...], lat[:D_LAT, here]).astype(BF16)
        kt[:D_NOPE, here] = both[:D_NOPE]
        vt[:, here] = both[D_NOPE:]
        kt[D_NOPE:, here] = lat[D_LAT:, here]

    down = lax.broadcasted_iota(jnp.int32, (STRIPE, rows), 0)
    along = lax.broadcasted_iota(jnp.int32, (1, STRIPE), 1)
    per = rows // STRIPE

    def scores_of(s):
        here = at(s, rows, rows)
        keys, vals = kt[:, here], vt[:, here]
        rel = pos[s] - down
        for t in range(nq // STRIPE):
            part = slice(t * STRIPE, (t + 1) * STRIPE)
            cut = (t % per) * STRIPE
            first = pos[put(seq, member_bits, t // per)][:, cut : cut + STRIPE] - along
            first = jnp.concatenate([first] * per, axis=1)
            got = jnp.where(rel <= first, nn(qall[part, :], keys), NEG)
            sc[part, here] = got
            dp[part, here] = nn(dall[part, :], vals)
            top = mx[part, :]
            for c in range(rows // LANE):
                top = jnp.maximum(top, got[:, c * LANE : (c + 1) * LANE])
            mx[part, :] = top

    def block_of(mask):
        by_core[mask].wait_recv()
        by_both[mask].wait_recv()
        keys_of(xor(seq, mask))
        scores_of(xor(seq, mask))

    keys_of(seq)
    for mask in levels[0]:
        relay(mask)
    for copy in q_got:
        copy.wait_recv()
    qall[...] = qd[:D_QK, :].T
    dall[...] = qd[D_QK:, :].T
    for mask in levels[0]:
        relay_y(mask)
    for copy in pos_got:
        copy.wait_recv()
    scores_of(seq)
    for mask in levels[1]:
        relay(mask)
    for mask in levels[0]:
        block_of(mask)
    for k in range(1, nb):
        if k + 1 < nb:
            for mask in levels[k + 1]:
                relay(mask)
        for mask in levels[k]:
            relay_y(mask)
        for mask in levels[k]:
            block_of(mask)

    factor = scale * LOG2E
    for t in range(nq // STRIPE):
        part = slice(t * STRIPE, (t + 1) * STRIPE)
        top = jnp.max(mx[part, :], axis=1, keepdims=True) * factor

        def sums(k, carry):
            total, weighted = carry
            here = at(k, LANE, LANE)
            e = jnp.exp2(sc[part, here] * factor - top)
            sc[part, here] = e
            return total + e, weighted + e * dp[part, here]

        zero = jnp.zeros((STRIPE, LANE), F32)
        total, weighted = loop(nk // LANE, sums, (zero, zero))
        total = jnp.sum(total, axis=1, keepdims=True)
        weighted = jnp.sum(weighted, axis=1, keepdims=True)
        inv = 1.0 / total
        sinv[part, :] = jnp.broadcast_to(inv, (STRIPE, LANE))
        sdel[part, :] = jnp.broadcast_to(weighted * inv, (STRIPE, LANE))

        def norm(k, carry):
            here = at(k, LANE, LANE)
            prob = sc[part, here] * sinv[part, :]
            sc[part, here] = prob
            pr[part, here] = prob.astype(BF16)
            return carry

        loop(nk // LANE, norm, 0)

    tile = math.gcd(nk, 512)

    def values_grad(k, carry):
        here = at(k, tile, tile)
        kvg[D_NOPE:, here] = nn(qd[D_QK:, :], pr[:, here]).astype(BF16)
        return carry

    loop(nk // tile, values_grad, 0)
    up[0] = nt(lat[:D_LAT, :], kvg[D_NOPE:, :]).astype(BF16)

    share = D_LAT // groups
    piece = share // subs

    summed, moved = {}, {}

    def source(a, i, g):
        return up.at[a, at(g * subs + i, piece, piece)]

    def place(i, s):
        return (
            at(pick(s, group_bits) * subs + i, piece, piece),
            at(pick(s, member_bits), LANE, LANE),
        )

    def sum_start(a, i, k=0, slot=0):
        bits = group_bits[::-1]
        if k == len(bits):
            return
        b, rest = bits[k], bits[k + 1 :]
        summed[a, i] = []
        for values in itertools.product((0, 1), repeat=len(rest)):
            to, own = flip(seq, b), seq
            for r, value in zip(rest, values):
                to = to + (1 << r) * (value - bit(to, r))
                own = own + (1 << r) * (value - bit(own, r))
            copy = sems.copy(
                source(a, i, pick(to, group_bits)), ur.at[a, i, slot], on_seq(flip(seq, b))
            )
            summed[a, i].append((copy, slot, pick(own, group_bits)))
            slot += 1

    def sum_end(a, i):
        slot = 0
        for k in range(len(group_bits)):
            for copy, slot, g in summed[a, i]:
                copy.wait_recv()
                kept = source(a, i, g)
                kept[...] = (kept[...].astype(F32) + ur[a, i, slot].astype(F32)).astype(BF16)
            sum_start(a, i, k + 1, slot + 1)

    def spread(a, i, mask, bits):
        r, c = place(i, xor(seq, mask))
        piece_at = fin.at[a, r, c]
        for b in bits:
            moved[a, i, mask | (1 << b)] = sems.copy(
                piece_at if mask else source(a, i, w), piece_at, on_seq(flip(seq, b))
            )

    def spread_z(a, i, mask):
        last = max([k for k, b in enumerate(zbits) if (mask >> b) & 1], default=-1)
        spread(a, i, mask, zbits[last + 1 :])

    def spread_x(a, i, mask):
        spread(a, i, mask, [0])

    def arrive(a, i, mask):
        moved[a, i, mask].wait_recv()

    def finish(a, i, mask):
        r, c = place(i, xor(seq, mask))
        got = fin[a, r, c] if mask else source(a, i, w)[...]
        (dk_ref if a else dv_ref)[r, c] = got.astype(F32)

    for i in range(subs):
        sum_start(0, i)

    for t in range(nq // STRIPE):
        part = slice(t * STRIPE, (t + 1) * STRIPE)

        def scored(k, carry):
            here = at(k, LANE, LANE)
            ds[part, here] = (
                sc[part, here] * (dp[part, here] - sdel[part, :]) * scale
            ).astype(BF16)
            return carry

        loop(nk // LANE, scored, 0)

    def keys_grad(k, carry):
        here = at(k, tile, tile)
        got = nn(qd[:D_QK, :], ds[:, here]).astype(BF16)
        kvg[:D_NOPE, here] = got[:D_NOPE]
        rp[:, here] = got[D_NOPE:]
        return carry

    loop(nk // tile, keys_grad, 0)
    up[1] = nt(lat[:D_LAT, :], kvg[:D_NOPE, :]).astype(BF16)
    for i in range(subs):
        sum_start(1, i)

    zmasks = list(range(1, nz))[::-1] + [0]
    to_core, to_y, to_x, to_z = {}, {}, {}, {}
    mine, others = y * 2 + core, (1 - y) * 2 + core

    def fold(k):
        here = at(xor(z, k), 2 * rows, 2 * rows)
        got = nn(kuv[...], kvg[:, here]).astype(BF16)
        got = jnp.concatenate([got, rp[:, here]], axis=0)
        for h in range(nhead):
            lg[h, k] = got[h * sub : (h + 1) * sub]
        to_core[k] = [
            sems.copy(lg.at[t * 2 + 1 - core, k], rc.at[j, k], other)
            for j, t in ((0, 1 - y), (1, y))
        ]

    def add_core(k):
        to_core[k][0].wait_recv()
        lg[others, k] = (lg[others, k].astype(F32) + rc[0, k].astype(F32)).astype(BF16)
        to_y[k] = sems.copy(lg.at[others, k], ry.at[k], across)
        to_core[k][1].wait_recv()
        lg[mine, k] = (lg[mine, k].astype(F32) + rc[1, k].astype(F32)).astype(BF16)

    def add_y(k):
        to_y[k].wait_recv()
        lg[mine, k] = (lg[mine, k].astype(F32) + ry[k].astype(F32)).astype(BF16)
        to_x[k] = sems.copy(
            lg.at[mine, k, :, at(1 - x, rows, rows)], rx.at[k], on_seq(flip(seq, 0))
        )

    def add_x(k):
        to_x[k].wait_recv()
        kept = lg[mine, k, :, at(x, rows, rows)].astype(F32) + rx[k].astype(F32)
        ac[k] = kept.astype(BF16)
        if k:
            to_z[k] = sems.copy(ac.at[k], rz.at[k], on_seq(xor(seq, 2 * k)))

    chunks = [(a, i) for a in range(2) for i in range(subs)]
    values, keys = chunks[:subs], chunks[subs:]
    zmoves = [m for m in masks if not m & 1]
    near_z = [m for m in zmoves if m.bit_count() == 1]
    far_z = [m for m in zmoves if m.bit_count() > 1]

    for k in zmasks:
        fold(k)
    for a, i in values:
        sum_end(a, i)
        spread_z(a, i, 0)
        spread_x(a, i, 0)
    dqt[...] = nt(kt[...], ds[...]).astype(BF16)
    for a, i in keys:
        sum_end(a, i)
        spread_z(a, i, 0)
        spread_x(a, i, 0)
    for k in zmasks:
        add_core(k)
    dq_in = []
    for v in range(1, heads):
        mask = sum(((v >> k) & 1) << b for k, b in enumerate(member_bits))
        there = xor(seq, mask)
        dq_in.append(
            sems.copy(
                dqt.at[:, at(pick(there, member_bits), rows, rows)], dqr.at[u], on_seq(there)
            )
        )
    dqr[u] = dqt[:, at(u, rows, rows)]
    for chunk in chunks:
        finish(*chunk, 0)
    late = []
    for k, mask in enumerate(near_z):
        for chunk in chunks:
            arrive(*chunk, mask)
            spread_z(*chunk, mask)
            if k == 0:
                spread_x(*chunk, mask)
            else:
                late.append((*chunk, mask))
            finish(*chunk, mask)
    for k in zmasks[:-1]:
        add_y(k)
    for k in zmasks[:1]:
        add_x(k)
    for move in late[: len(late) // 2]:
        spread_x(*move)
    late = late[len(late) // 2 :]
    for k in zmasks[-1:]:
        add_y(k)
    for k in zmasks[1:-1]:
        add_x(k)
    for mask in far_z:
        for chunk in chunks:
            arrive(*chunk, mask)
            spread_z(*chunk, mask)
            late.append((*chunk, mask))
    for move in late:
        spread_x(*move)
        if move[2] in far_z:
            finish(*move)
    add_x(0)
    total = ac[0].astype(F32)
    for k in zmasks[:-1]:
        to_z[k].wait_recv()
        total = total + rz[k].astype(F32)
    fl[head] = total.astype(BF16)
    first = sems.copy(fl.at[head], fl.at[head], across)
    second = sems.copy(fl.at[head], fl.at[head], other)
    for copy in dq_in:
        copy.wait_recv()
    for h in range(heads):
        dq_ref[:, h * D_QK : (h + 1) * D_QK] = dqr[h].T
    first.wait_recv()
    third = sems.copy(fl.at[others], fl.at[others], other)
    for mask in [0] + zmoves:
        for chunk in chunks:
            arrive(*chunk, mask | 1)
            finish(*chunk, mask | 1)
    second.wait_recv()
    third.wait_recv()
    for h in range(nhead):
        dl_ref[h * sub : (h + 1) * sub, :] = fl[h].astype(F32)
    for copy in sems.sent:
        copy.wait_send()


def store(*refs):
    sems = refs[8]
    copies = [pltpu.make_async_copy(refs[k], refs[4 + k], sems.at[k]) for k in range(4)]
    for copy in copies:
        copy.start()
    for copy in copies:
        copy.wait()


def make_shards(nseq, nhead):
    def shards(queries, latents, key_up, value_up, out_grad, positions):
        rows, heads = latents.shape[0], key_up.shape[1] // D_NOPE
        nq, nk = heads * rows, nseq * rows
        nz, groups = nseq // 2, nseq // heads
        subs = 2
        share = D_LAT // groups
        sub = D_ALL // nhead
        cols = key_up.shape[1]
        copies = (nseq - 1) * 5 + 2 * (heads - 1)
        copies += 2 * subs * (groups - 1 + nseq - 1) + 5 * nz + 3
        vmem = pl.BlockSpec(memory_space=pltpu.VMEM)
        body = lambda *refs: kernel(nseq, nhead, subs, *refs)
        moved = [
            (queries.shape, BF16),
            ((D_ALL, rows), BF16),
            (out_grad.shape, BF16),
            ((1, rows), jnp.int32),
        ]
        scratch = [
            ((heads, D_QK + D_V, rows), BF16),
            ((D_QK + D_V, nq), BF16),
            ((nq, D_QK), BF16),
            ((nq, D_V), BF16),
            ((D_ALL, nk), BF16),
            ((nseq, 1, rows), jnp.int32),
            ((D_QK, nk), BF16),
            ((D_V, nk), BF16),
            ((D_LAT, D_NOPE + D_V), BF16),
            ((D_NOPE + D_V, D_LAT), BF16),
            ((nq, nk), F32),
            ((nq, nk), F32),
            ((nq, LANE), F32),
            ((nq, LANE), F32),
            ((nq, LANE), F32),
            ((nq, nk), BF16),
            ((nq, nk), BF16),
            ((D_NOPE + D_V, nk), BF16),
            ((D_ROPE, nk), BF16),
            ((2, D_LAT, LANE), BF16),
            ((2, subs, max(groups - 1, 1), share // subs, LANE), BF16),
            ((2, D_LAT, cols), BF16),
            ((nhead, nz, sub, 2 * rows), BF16),
            ((nhead // 2, nz, sub, 2 * rows), BF16),
            ((nz, sub, 2 * rows), BF16),
            ((nz, sub, rows), BF16),
            ((nz, sub, rows), BF16),
            ((nz, sub, rows), BF16),
            ((nhead, sub, rows), BF16),
            ((D_QK, nq), BF16),
            ((heads, D_QK, rows), BF16),
        ]
        limit = 8 * 1024 * 1024
        for shape, dtype in moved + scratch:
            padded = (-(-shape[-1] // LANE) * LANE) * (-(-shape[-2] // 16) * 16)
            limit += math.prod(shape[:-2]) * padded * jnp.dtype(dtype).itemsize
        dq, dl, dk, dv = pl.pallas_call(
            body,
            out_shape=(
                jax.ShapeDtypeStruct(queries.shape, BF16),
                jax.ShapeDtypeStruct((D_ALL, rows), F32),
                jax.ShapeDtypeStruct(key_up.shape, F32),
                jax.ShapeDtypeStruct(value_up.shape, F32),
            ),
            in_specs=[pl.BlockSpec(memory_space=pltpu.HBM)] * 6,
            out_specs=(vmem,) * 4,
            scratch_shapes=[pltpu.VMEM(shape, dtype) for shape, dtype in moved]
            + [pltpu.SemaphoreType.DMA((6,))]
            + [pltpu.VMEM(shape, dtype) for shape, dtype in scratch]
            + [pltpu.SemaphoreType.DMA((copies,)), pltpu.SemaphoreType.DMA((copies,))],
            compiler_params=pltpu.CompilerParams(
                collective_id=0, has_side_effects=True, vmem_limit_bytes=min(limit, 60 * 1024 * 1024)
            ),
        )(*[
            pltpu.with_memory_space_constraint(a, pltpu.HBM)
            for a in (queries, latents.T, key_up, value_up, out_grad, positions[None, :])
        ])
        done = (dq, dl, dk, dv)
        dq, dl, dk, dv = pl.pallas_call(
            store,
            out_shape=[jax.ShapeDtypeStruct(a.shape, a.dtype) for a in done],
            in_specs=[vmem] * 4,
            out_specs=[pl.BlockSpec(memory_space=pltpu.HBM)] * 4,
            scratch_shapes=[pltpu.SemaphoreType.DMA((4,))],
            compiler_params=pltpu.CompilerParams(vmem_limit_bytes=1024 * 1024),
        )(*done)
        return dq, dl.T, dk, dv

    return shards


def solution(mesh):
    in_specs = (
        P("seq", "head"),
        P("seq", None),
        P(None, "head"),
        P(None, "head"),
        P("seq", "head"),
        P("seq"),
    )
    out_specs = (P("seq", "head"), P("seq", None), P(None, "head"), P(None, "head"))
    shards = make_shards(mesh.shape["seq"], mesh.shape["head"])
    return jax.shard_map(shards, mesh=mesh, in_specs=in_specs, out_specs=out_specs, check_vma=False)
```

```python
import itertools
import math

import jax
import jax.numpy as jnp
from jax import lax
from jax.experimental import pallas as pl
from jax.experimental.pallas import tpu as pltpu
from jax.sharding import PartitionSpec as P

D_LAT = 512
D_ROPE = 64
D_NOPE = 128
D_V = 128
D_QK = D_NOPE + D_ROPE
D_ALL = D_LAT + D_ROPE
LANE = 128
STRIPE = 128
NEG = -1e30
LOG2E = 1.4426950408889634
MESH = pl.DeviceIdType.MESH
F32 = jnp.float32
BF16 = jnp.bfloat16


def bit(index, b):
    return (index // (1 << b)) % 2


def flip(index, b):
    return index + (1 << b) * (1 - 2 * bit(index, b))


def xor(index, mask):
    b = 0
    while mask >> b:
        if (mask >> b) & 1:
            index = flip(index, b)
        b += 1
    return index


def pick(index, bits):
    out = 0
    for k, b in enumerate(bits):
        out = out + (1 << k) * bit(index, b)
    return out


def put(index, bits, value):
    for k, b in enumerate(bits):
        index = index + (1 << b) * (((value >> k) & 1) - bit(index, b))
    return index


def nn(a, b):
    return lax.dot_general(a, b, (((1,), (0,)), ((), ())), preferred_element_type=F32)


def nt(a, b):
    return lax.dot_general(a, b, (((1,), (1,)), ((), ())), preferred_element_type=F32)


def loop(n, body, init):
    if n <= 8:
        for t in range(n):
            init = body(t, init)
        return init
    return lax.fori_loop(0, n, body, init)


def when(only, act):
    if only is None:
        act()
    else:
        pl.when(only)(act)


class Sems:
    def __init__(self, send, recv):
        self.send, self.recv, self.used = send, recv, 0
        self.sent = []

    def copy(self, src, dst, device, only=None):
        k = self.used
        self.used += 1
        copy = pltpu.make_async_remote_copy(
            src_ref=src,
            dst_ref=dst,
            send_sem=self.send.at[k],
            recv_sem=self.recv.at[k],
            device_id=device,
            device_id_type=MESH,
        )
        when(only, copy.start)
        self.sent.append((only, copy))
        return copy


def kernel(
    nseq, nhead, subs,
    q_in, lat_in, ku_in, vu_in, do_in, pos_in,
    dq_ref, dl_ref, dk_ref, dv_ref,
    q_ref, lat_ref, do_ref, pos_ref, load,
    stage, qd, qall, dall, lat, pos, kt, vt, kuv, ut, sc, dp, mx, sinv, sdel,
    pr, ds, kvg, rp, up, ur, ug, fin, lg, rc, ry, rx, ac, rz, fl, dqt, dqr,
    send, recv,
):
    seq, head = lax.axis_index("seq"), lax.axis_index("head")
    rows = lat_in.shape[1]
    heads = ku_in.shape[1] // D_NOPE
    nq, nk = heads * rows, nseq * rows
    nb = nseq.bit_length() - 1
    hb = heads.bit_length() - 1
    slot_bits = list(range(1, 1 + hb))
    group_bits = list(range(1 + hb, nb))
    groups = 1 << len(group_bits)
    nz = nseq // 2
    scale = 1.0 / math.sqrt(D_QK)
    sems = Sems(send, recv)
    u, w = pick(seq, slot_bits), pick(seq, group_bits)
    x, z = bit(seq, 0), seq // 2
    core, y = bit(head, 0), bit(head, 1)
    active, passive = core == x, core != x

    def on_seq(s):
        return (s, head)

    def on_head(h):
        return (seq, h)

    other = on_head(flip(head, 0))
    across = on_head(flip(head, 1))

    barrier = pltpu.get_barrier_semaphore()
    for mask in range(1, nseq):
        pl.semaphore_signal(barrier, inc=1, device_id=on_seq(xor(seq, mask)), device_id_type=MESH)
    for device in (other, across):
        pl.semaphore_signal(barrier, inc=1, device_id=device, device_id_type=MESH)

    def swap(k):
        return (xor(seq, 2 * k) + core - x, head + x - core)

    def greet(k):
        pl.semaphore_signal(barrier, inc=1, device_id=swap(k), device_id_type=MESH)

    for k in range(1, heads):
        greet(k)
    when(passive, lambda: greet(0))

    def at(start, size, step):
        return pl.ds(pl.multiple_of(start * step, step), size)

    mine_k, mine_v = at(u, D_NOPE, D_NOPE), at(u, D_V, D_V)
    loads = [
        pltpu.make_async_copy(src, dst, load.at[k])
        for k, (src, dst) in enumerate((
            (lat_in, lat_ref),
            (q_in, q_ref),
            (do_in, do_ref),
            (pos_in, pos_ref),
            (ku_in.at[:, mine_k], kuv.at[:, :D_NOPE]),
            (vu_in.at[:, mine_v], kuv.at[:, D_NOPE:]),
        ))
    ]
    for copy in loads[:4]:
        copy.start()
    for copy in loads[4:]:
        when(active, copy.start)
    mx[...] = jnp.full(mx.shape, NEG, F32)

    zbits = list(range(nb - 1, 0, -1))
    order = zbits + [0]
    masks = [
        sum(1 << b for b in some)
        for size in range(1, nb + 1)
        for some in itertools.combinations(order, size)
    ]
    zmoves = [m for m in masks if not m & 1]
    by_seq, by_core, by_y, by_both = {}, {}, {}, {}
    sub = D_ALL // nhead

    def quarter(h, s):
        return lat.at[at(h, sub, sub), at(s, rows, rows)]

    def forward(mask):
        piece = quarter(head, xor(seq, mask))
        source = piece if mask else lat_ref.at[at(head, sub, sub)]
        for to in [1] if mask else zmoves + [1]:
            by_seq[mask | to] = sems.copy(source, piece, on_seq(xor(seq, to)))

    def relay(mask):
        by_seq[mask].wait_recv()
        if not mask & 1:
            forward(mask)
        piece = quarter(head, xor(seq, mask))
        by_y[mask] = sems.copy(piece, piece, across)
        by_core[mask] = sems.copy(piece, piece, other)

    def relay_y(mask):
        by_y[mask].wait_recv()
        piece = quarter(flip(head, 1), xor(seq, mask))
        by_both[mask] = sems.copy(piece, piece, other)

    loads[0].wait()
    pl.semaphore_wait(barrier, nseq + heads + (core - x) * (core - x))
    forward(0)
    loads[3].wait()
    pos_got = [
        sems.copy(pos_ref, pos.at[seq], on_seq(xor(seq, mask))) for mask in range(1, nseq)
    ]
    for copy in loads[1:3]:
        copy.wait()
    for h in range(heads):
        stage[h, :D_QK, :] = q_ref[:, h * D_QK : (h + 1) * D_QK].T
        stage[h, D_QK:, :] = do_ref[:, h * D_V : (h + 1) * D_V].T
    q_got = {}
    for k in range(heads):
        q_got[k] = sems.copy(
            stage.at[pick(xor(seq, 2 * k), slot_bits)],
            qd.at[:, at(u, rows, rows)],
            swap(k),
            None if k else passive,
        )
    for copy in loads[4:]:
        when(active, copy.wait)
    kuv_got = sems.copy(kuv, kuv, other, active)
    lat[:, at(seq, rows, rows)] = lat_ref[...]
    pos[seq] = pos_ref[...]

    @pl.when(active)
    def _():
        qd[:, at(u, rows, rows)] = stage[u]

    def keys_of(s):
        here = at(s, rows, rows)
        both = nn(ut[...], lat[:D_LAT, here]).astype(BF16)
        kt[:D_NOPE, here] = both[:D_NOPE]
        vt[:, here] = both[D_NOPE:]
        kt[D_NOPE:, here] = lat[D_LAT:, here]

    down = lax.broadcasted_iota(jnp.int32, (STRIPE, rows), 0)
    per = rows // STRIPE
    lane = jnp.concatenate([lax.broadcasted_iota(jnp.int32, (1, STRIPE), 1)] * per, axis=1)

    def scores_of(s, k):
        here = at(s, rows, rows)
        keys, vals = kt[:, here], vt[:, here]
        rel = pos[s] - down
        first = pos[xor(seq, 2 * k) + core - x] - lane
        slot = pick(xor(seq, 2 * k), slot_bits)
        for t in range(per):
            part = at(slot * per + t, STRIPE, STRIPE)
            base = first[:, t * STRIPE : (t + 1) * STRIPE]
            base = jnp.concatenate([base] * per, axis=1)
            got = jnp.where(rel <= base, nn(qall[part, :], keys), NEG)
            sc[part, here] = got
            dp[part, here] = nn(dall[part, :], vals)
            top = mx[part, :]
            for c in range(rows // LANE):
                top = jnp.maximum(top, got[:, c * LANE : (c + 1) * LANE])
            mx[part, :] = top

    def turn(k):
        if k:
            q_got[k].wait_recv()
        else:
            when(passive, q_got[0].wait_recv)
        here = at(pick(xor(seq, 2 * k), slot_bits), rows, rows)
        qall[here, :] = qd[:D_QK, here].T
        dall[here, :] = qd[D_QK:, here].T

    def block_of(mask):
        by_core[mask].wait_recv()
        by_both[mask].wait_recv()
        keys_of(xor(seq, mask))

    for mask in zmoves + [1]:
        relay(mask)
    when(passive, kuv_got.wait_recv)
    ut[...] = kuv[...].T
    keys_of(seq)
    for mask in zmoves:
        relay(mask | 1)
    for mask in zmoves + [1]:
        relay_y(mask)
    for copy in pos_got:
        copy.wait_recv()
    for k in range(heads // 2):
        turn(k)
    for mask in zmoves + [1]:
        block_of(mask)
    for mask in zmoves:
        relay_y(mask | 1)
    early = [0] + zmoves + [1]
    for mask in early:
        for k in range(heads // 2):
            scores_of(xor(seq, mask), k)
    for mask in zmoves:
        block_of(mask | 1)
    for mask in zmoves:
        for k in range(heads // 2):
            scores_of(xor(seq, mask | 1), k)
    for k in range(heads // 2, heads):
        turn(k)
        for mask in [0] + masks:
            scores_of(xor(seq, mask), k)

    first_sent, sems.sent = sems.sent, []

    def drain(sent):
        for only in (None, active, passive):
            some = [copy for kind, copy in sent if kind is only]

            def act():
                for copy in some:
                    copy.wait_send()

            if some:
                when(only, act)

    factor = scale * LOG2E
    for t in range(nq // STRIPE):
        part = slice(t * STRIPE, (t + 1) * STRIPE)
        top = jnp.max(mx[part, :], axis=1, keepdims=True) * factor

        def sums(k, carry):
            total, weighted = carry
            here = at(k, LANE, LANE)
            e = jnp.exp2(sc[part, here] * factor - top)
            sc[part, here] = e
            return total + e, weighted + e * dp[part, here]

        zero = jnp.zeros((STRIPE, LANE), F32)
        total, weighted = loop(nk // LANE, sums, (zero, zero))
        total = jnp.sum(total, axis=1, keepdims=True)
        weighted = jnp.sum(weighted, axis=1, keepdims=True)
        inv = 1.0 / total
        sinv[part, :] = jnp.broadcast_to(inv, (STRIPE, LANE))
        sdel[part, :] = jnp.broadcast_to(weighted * inv, (STRIPE, LANE))

        def norm(k, carry):
            here = at(k, LANE, LANE)
            prob = sc[part, here] * sinv[part, :]
            sc[part, here] = prob
            pr[part, here] = prob.astype(BF16)
            return carry

        loop(nk // LANE, norm, 0)

    tile = math.gcd(nk, 512)

    def values_grad(k, carry):
        here = at(k, tile, tile)
        kvg[D_NOPE:, here] = nn(qd[D_QK:, :], pr[:, here]).astype(BF16)
        return carry

    loop(nk // tile, values_grad, 0)
    up[0] = nt(lat[:D_LAT, :], kvg[D_NOPE:, :]).astype(BF16)

    share = D_LAT // groups
    piece = share // subs

    summed, moved = {}, {}

    def source(a, i, g):
        return up.at[a, at(g * subs + i, piece, piece)]

    def place(i, s):
        return (
            at(pick(s, group_bits) * subs + i, piece, piece),
            at(pick(s, slot_bits), LANE, LANE),
        )

    def sum_start(a, i):
        for g in range(groups):
            part = at(g * subs + i, piece, piece)
            summed[a, i, g] = sems.copy(up.at[a, part], ur.at[a, part], other, passive)

    def add_up(a, i, g, ref):
        def act():
            kept = source(a, i, g)
            kept[...] = (kept[...].astype(F32) + ref[...].astype(F32)).astype(BF16)

        when(active, act)

    def sum_end(a, i):
        for g in range(groups):
            when(active, summed[a, i, g].wait_recv)
            add_up(a, i, g, ur.at[a, at(g * subs + i, piece, piece)])
        bits, slot = group_bits[::-1], 0
        for k, b in enumerate(bits):
            rest, copies = bits[k + 1 :], []
            for values in itertools.product((0, 1), repeat=len(rest)):
                to, own = flip(seq, b), seq
                for r, value in zip(rest, values):
                    to = to + (1 << r) * (value - bit(to, r))
                    own = own + (1 << r) * (value - bit(own, r))
                copy = sems.copy(
                    source(a, i, pick(to, group_bits)),
                    ug.at[a, i, slot],
                    on_seq(flip(seq, b)),
                    active,
                )
                copies.append((copy, slot, pick(own, group_bits)))
                slot += 1
            for copy, at_slot, g in copies:
                when(active, copy.wait_recv)
                add_up(a, i, g, ug.at[a, i, at_slot])

    def spread(a, i, mask, bits):
        r, c = place(i, xor(seq, mask))
        piece_at = fin.at[a, r, c]
        for b in bits:
            moved[a, i, mask | (1 << b)] = sems.copy(
                piece_at if mask else source(a, i, w), piece_at, on_seq(flip(seq, b)), active
            )

    def spread_z(a, i, mask):
        last = max([k for k, b in enumerate(zbits) if (mask >> b) & 1], default=-1)
        spread(a, i, mask, zbits[last + 1 :])

    def spread_x(a, i, mask):
        spread(a, i, mask, [0])

    def arrive(a, i, mask):
        when(passive if mask & 1 else active, moved[a, i, mask].wait_recv)

    def finish(a, i, mask):
        r, c = place(i, xor(seq, mask))

        def act():
            got = fin[a, r, c] if mask else source(a, i, w)[...]
            (dk_ref if a else dv_ref)[r, c] = got.astype(F32)

        when(passive if mask & 1 else active, act)

    for i in range(subs):
        sum_start(0, i)

    for t in range(nq // STRIPE):
        part = slice(t * STRIPE, (t + 1) * STRIPE)

        def scored(k, carry):
            here = at(k, LANE, LANE)
            ds[part, here] = (
                sc[part, here] * (dp[part, here] - sdel[part, :]) * scale
            ).astype(BF16)
            return carry

        loop(nk // LANE, scored, 0)

    for i in range(subs):
        sum_end(0, i)
        spread_z(0, i, 0)
        spread_x(0, i, 0)
    def keys_grad(k, carry):
        here = at(k, tile, tile)
        got = nn(qd[:D_QK, :], ds[:, here]).astype(BF16)
        kvg[:D_NOPE, here] = got[:D_NOPE]
        rp[:, here] = got[D_NOPE:]
        return carry

    loop(nk // tile, keys_grad, 0)

    zmasks = list(range(1, nz))[::-1] + [0]
    to_core, to_y, to_x, to_z = {}, {}, {}, {}
    mine, others = y * 2 + core, (1 - y) * 2 + core

    def fold(k):
        here = at(xor(z, k), 2 * rows, 2 * rows)
        got = nn(kuv[...], kvg[:, here]).astype(BF16)
        got = jnp.concatenate([got, rp[:, here]], axis=0)
        for h in range(nhead):
            lg[h, k] = got[h * sub : (h + 1) * sub]
        to_core[k] = [
            sems.copy(lg.at[t * 2 + 1 - core, k], rc.at[j, k], other)
            for j, t in ((0, 1 - y), (1, y))
        ]

    def add_core(k):
        to_core[k][0].wait_recv()
        lg[others, k] = (lg[others, k].astype(F32) + rc[0, k].astype(F32)).astype(BF16)
        to_y[k] = sems.copy(lg.at[others, k], ry.at[k], across)
        to_core[k][1].wait_recv()
        lg[mine, k] = (lg[mine, k].astype(F32) + rc[1, k].astype(F32)).astype(BF16)

    def add_y(k):
        to_y[k].wait_recv()
        lg[mine, k] = (lg[mine, k].astype(F32) + ry[k].astype(F32)).astype(BF16)
        to_x[k] = sems.copy(
            lg.at[mine, k, :, at(1 - x, rows, rows)], rx.at[k], on_seq(flip(seq, 0))
        )

    def add_x(k):
        to_x[k].wait_recv()
        kept = lg[mine, k, :, at(x, rows, rows)].astype(F32) + rx[k].astype(F32)
        ac[k] = kept.astype(BF16)
        if k:
            to_z[k] = sems.copy(ac.at[k], rz.at[k], on_seq(xor(seq, 2 * k)))

    chunks = [(a, i) for a in range(2) for i in range(subs)]
    values, keys = chunks[:subs], chunks[subs:]
    near_z = [m for m in zmoves if m.bit_count() == 1]
    far_z = [m for m in zmoves if m.bit_count() > 1]

    for k in zmasks:
        fold(k)
    up[1] = nt(lat[:D_LAT, :], kvg[:D_NOPE, :]).astype(BF16)
    for i in range(subs):
        sum_start(1, i)
    for k in zmasks:
        add_core(k)
    for a, i in keys:
        sum_end(a, i)
        spread_z(a, i, 0)
        spread_x(a, i, 0)
    for chunk in chunks:
        finish(*chunk, 0)

    held = []

    def along_z(some, mask, hold=False):
        for chunk in some:
            arrive(*chunk, mask)
            spread_z(*chunk, mask)
            if hold:
                held.append((*chunk, mask))
            else:
                spread_x(*chunk, mask)
            finish(*chunk, mask)

    dqt[...] = nt(kt[...], ds[...]).astype(BF16)
    for mask in near_z[1:][::-1]:
        along_z(values, mask)
    drain(first_sent)
    for k in zmasks[:-3]:
        add_y(k)
    for mask in near_z[1:][::-1]:
        along_z(keys, mask)
    for k in zmasks[-3:-2]:
        add_y(k)
    along_z(values, near_z[0])
    for k in zmasks[-2:-1]:
        add_y(k)
    along_z(keys, near_z[0], True)
    for k in zmasks[:1]:
        add_x(k)
    for k in zmasks[-1:]:
        add_y(k)
    for move in held:
        spread_x(*move)
    dq_in = [
        sems.copy(
            dqt.at[:, at(pick(xor(seq, 2 * k), slot_bits), rows, rows)],
            dqr.at[u],
            swap(k),
            None if k else passive,
        )
        for k in range(heads)
    ]

    @pl.when(active)
    def _():
        dqr[u] = dqt[:, at(u, rows, rows)]

    for k in zmasks[1:-1]:
        add_x(k)
    last_sent, sems.sent = sems.sent, []
    for mask in far_z:
        along_z(chunks, mask)
    add_x(0)
    total = ac[0].astype(F32)
    for k in zmasks[:-1]:
        to_z[k].wait_recv()
        total = total + rz[k].astype(F32)
    fl[head] = total.astype(BF16)
    first = sems.copy(fl.at[head], fl.at[head], across)
    second = sems.copy(fl.at[head], fl.at[head], other)
    drain(last_sent)
    for copy in dq_in[1:]:
        copy.wait_recv()
    when(passive, dq_in[0].wait_recv)
    for h in range(heads):
        dq_ref[:, h * D_QK : (h + 1) * D_QK] = dqr[h].T
    first.wait_recv()
    third = sems.copy(fl.at[others], fl.at[others], other)
    for mask in [0] + zmoves:
        for chunk in chunks:
            arrive(*chunk, mask | 1)
            finish(*chunk, mask | 1)
    second.wait_recv()
    third.wait_recv()
    for h in range(nhead):
        dl_ref[h * sub : (h + 1) * sub, :] = fl[h].astype(F32)
    drain(sems.sent)


def store(*refs):
    sems = refs[8]
    copies = [pltpu.make_async_copy(refs[k], refs[4 + k], sems.at[k]) for k in range(4)]
    for copy in copies:
        copy.start()
    for copy in copies:
        copy.wait()


def make_shards(nseq, nhead):
    def shards(queries, latents, key_up, value_up, out_grad, positions):
        rows, heads = latents.shape[0], key_up.shape[1] // D_NOPE
        nq, nk = heads * rows, nseq * rows
        nz, groups = nseq // 2, nseq // (2 * heads)
        subs = 2
        share = D_LAT // groups
        sub = D_ALL // nhead
        cols = key_up.shape[1]
        copies = (nseq - 1) * 5 + 2 * heads + 1
        copies += 2 * subs * (2 * groups - 1 + nseq - 1) + 5 * nz + 3
        vmem = pl.BlockSpec(memory_space=pltpu.VMEM)
        body = lambda *refs: kernel(nseq, nhead, subs, *refs)
        moved = [
            (queries.shape, BF16),
            ((D_ALL, rows), BF16),
            (out_grad.shape, BF16),
            ((1, rows), jnp.int32),
        ]
        scratch = [
            ((heads, D_QK + D_V, rows), BF16),
            ((D_QK + D_V, nq), BF16),
            ((nq, D_QK), BF16),
            ((nq, D_V), BF16),
            ((D_ALL, nk), BF16),
            ((nseq, 1, rows), jnp.int32),
            ((D_QK, nk), BF16),
            ((D_V, nk), BF16),
            ((D_LAT, D_NOPE + D_V), BF16),
            ((D_NOPE + D_V, D_LAT), BF16),
            ((nq, nk), F32),
            ((nq, nk), F32),
            ((nq, LANE), F32),
            ((nq, LANE), F32),
            ((nq, LANE), F32),
            ((nq, nk), BF16),
            ((nq, nk), BF16),
            ((D_NOPE + D_V, nk), BF16),
            ((D_ROPE, nk), BF16),
            ((2, D_LAT, LANE), BF16),
            ((2, D_LAT, LANE), BF16),
            ((2, subs, max(groups - 1, 1), share // subs, LANE), BF16),
            ((2, D_LAT, cols), BF16),
            ((nhead, nz, sub, 2 * rows), BF16),
            ((nhead // 2, nz, sub, 2 * rows), BF16),
            ((nz, sub, 2 * rows), BF16),
            ((nz, sub, rows), BF16),
            ((nz, sub, rows), BF16),
            ((nz, sub, rows), BF16),
            ((nhead, sub, rows), BF16),
            ((D_QK, nq), BF16),
            ((heads, D_QK, rows), BF16),
        ]
        limit = 8 * 1024 * 1024
        for shape, dtype in moved + scratch:
            padded = (-(-shape[-1] // LANE) * LANE) * (-(-shape[-2] // 16) * 16)
            limit += math.prod(shape[:-2]) * padded * jnp.dtype(dtype).itemsize
        dq, dl, dk, dv = pl.pallas_call(
            body,
            out_shape=(
                jax.ShapeDtypeStruct(queries.shape, BF16),
                jax.ShapeDtypeStruct((D_ALL, rows), F32),
                jax.ShapeDtypeStruct(key_up.shape, F32),
                jax.ShapeDtypeStruct(value_up.shape, F32),
            ),
            in_specs=[pl.BlockSpec(memory_space=pltpu.HBM)] * 6,
            out_specs=(vmem,) * 4,
            scratch_shapes=[pltpu.VMEM(shape, dtype) for shape, dtype in moved]
            + [pltpu.SemaphoreType.DMA((6,))]
            + [pltpu.VMEM(shape, dtype) for shape, dtype in scratch]
            + [pltpu.SemaphoreType.DMA((copies,)), pltpu.SemaphoreType.DMA((copies,))],
            compiler_params=pltpu.CompilerParams(
                collective_id=0, has_side_effects=True, vmem_limit_bytes=min(limit, 60 * 1024 * 1024)
            ),
        )(*[
            pltpu.with_memory_space_constraint(a, pltpu.HBM)
            for a in (queries, latents.T, key_up, value_up, out_grad, positions[None, :])
        ])
        done = (dq, dl, dk, dv)
        dq, dl, dk, dv = pl.pallas_call(
            store,
            out_shape=[jax.ShapeDtypeStruct(a.shape, a.dtype) for a in done],
            in_specs=[vmem] * 4,
            out_specs=[pl.BlockSpec(memory_space=pltpu.HBM)] * 4,
            scratch_shapes=[pltpu.SemaphoreType.DMA((4,))],
            compiler_params=pltpu.CompilerParams(vmem_limit_bytes=1024 * 1024),
        )(*done)
        return dq, dl.T, dk, dv

    return shards


def solution(mesh):
    in_specs = (
        P("seq", "head"),
        P("seq", None),
        P(None, "head"),
        P(None, "head"),
        P("seq", "head"),
        P("seq"),
    )
    out_specs = (P("seq", "head"), P("seq", None), P(None, "head"), P(None, "head"))
    shards = make_shards(mesh.shape["seq"], mesh.shape["head"])
    return jax.shard_map(shards, mesh=mesh, in_specs=in_specs, out_specs=out_specs, check_vma=False)
```

```python
import itertools
import math

import jax
import jax.numpy as jnp
from jax import lax
from jax.experimental import pallas as pl
from jax.experimental.pallas import tpu as pltpu
from jax.sharding import PartitionSpec as P

D_LAT = 512
D_ROPE = 64
D_NOPE = 128
D_V = 128
D_QK = D_NOPE + D_ROPE
D_ALL = D_LAT + D_ROPE
LANE = 128
STRIPE = 128
NEG = -1e30
LOG2E = 1.4426950408889634
MESH = pl.DeviceIdType.MESH
F32 = jnp.float32
BF16 = jnp.bfloat16


def bit(index, b):
    return (index // (1 << b)) % 2


def flip(index, b):
    return index + (1 << b) * (1 - 2 * bit(index, b))


def xor(index, mask):
    b = 0
    while mask >> b:
        if (mask >> b) & 1:
            index = flip(index, b)
        b += 1
    return index


def pick(index, bits):
    out = 0
    for k, b in enumerate(bits):
        out = out + (1 << k) * bit(index, b)
    return out


def put(index, bits, value):
    for k, b in enumerate(bits):
        index = index + (1 << b) * (((value >> k) & 1) - bit(index, b))
    return index


def nn(a, b):
    return lax.dot_general(a, b, (((1,), (0,)), ((), ())), preferred_element_type=F32)


def nt(a, b):
    return lax.dot_general(a, b, (((1,), (1,)), ((), ())), preferred_element_type=F32)


def loop(n, body, init):
    if n <= 8:
        for t in range(n):
            init = body(t, init)
        return init
    return lax.fori_loop(0, n, body, init)


def when(only, act):
    if only is None:
        act()
    else:
        pl.when(only)(act)


class Sems:
    def __init__(self, send, recv):
        self.send, self.recv = send, recv
        self.sends, self.recvs, self.shared = 0, 0, {}
        self.sent = []

    def slots(self, group, arrive):
        if ("send", group) not in self.shared:
            if group is not None:
                self.shared["send", group] = self.sends
            out = self.sends
            self.sends += 1
        else:
            out = self.shared["send", group]
        if not arrive:
            into = self.recvs
            self.recvs += 1
        else:
            into = self.shared.setdefault(("recv", group), self.recvs)
            self.recvs = max(self.recvs, into + 1)
        return self.send.at[out], self.recv.at[into]

    def make(self, src, dst, device, group=None, arrive=False):
        send, recv = self.slots(group, arrive)
        return pltpu.make_async_remote_copy(
            src_ref=src,
            dst_ref=dst,
            send_sem=send,
            recv_sem=recv,
            device_id=device,
            device_id_type=MESH,
        )

    def copy(self, src, dst, device, only=None, group=None, arrive=False):
        copy = self.make(src, dst, device, group, arrive)
        when(only, copy.start)
        if group is None:
            self.sent.append((only, copy))
        return copy

    def whole(self, ref, device, group):
        send = self.send.at[self.shared["send", group]]
        recv = self.recv.at[self.shared.get(("recv", group), 0)]
        return pltpu.make_async_remote_copy(
            src_ref=ref,
            dst_ref=ref,
            send_sem=send,
            recv_sem=recv,
            device_id=device,
            device_id_type=MESH,
        )


def kernel(
    nseq, nhead, subs,
    q_in, lat_in, ku_in, vu_in, do_in, pos_in,
    dq_ref, dl_ref, dk_ref, dv_ref,
    q_ref, lat_ref, do_ref, pos_ref, load,
    stage, qd, qall, dall, lat, pos, kt, vt, kuv, ut, sc, dp, mx, sinv, sdel,
    pr, ds, kvg, rp, up, ur, ug, fin, lg, rc, ry, rx, ac, rz, fl, dqt, dqr,
    send, recv,
):
    seq, head = lax.axis_index("seq"), lax.axis_index("head")
    rows = lat_in.shape[1]
    heads = ku_in.shape[1] // D_NOPE
    nq, nk = heads * rows, nseq * rows
    nb = nseq.bit_length() - 1
    hb = heads.bit_length() - 1
    slot_bits = list(range(1, 1 + hb))
    group_bits = list(range(1 + hb, nb))
    groups = 1 << len(group_bits)
    nz = nseq // 2
    scale = 1.0 / math.sqrt(D_QK)
    sems = Sems(send, recv)
    u, w = pick(seq, slot_bits), pick(seq, group_bits)
    x, z = bit(seq, 0), seq // 2
    core, y = bit(head, 0), bit(head, 1)
    active, passive = core == x, core != x

    def on_seq(s):
        return (s, head)

    def on_head(h):
        return (seq, h)

    other = on_head(flip(head, 0))
    across = on_head(flip(head, 1))

    barrier = pltpu.get_barrier_semaphore()
    for mask in range(1, nseq):
        pl.semaphore_signal(barrier, inc=1, device_id=on_seq(xor(seq, mask)), device_id_type=MESH)
    for device in (other, across):
        pl.semaphore_signal(barrier, inc=1, device_id=device, device_id_type=MESH)

    def swap(k):
        return (xor(seq, 2 * k) + core - x, head + x - core)

    def greet(k):
        pl.semaphore_signal(barrier, inc=1, device_id=swap(k), device_id_type=MESH)

    for k in range(1, heads):
        greet(k)
    when(passive, lambda: greet(0))

    def at(start, size, step):
        return pl.ds(pl.multiple_of(start * step, step), size)

    mine_k, mine_v = at(u, D_NOPE, D_NOPE), at(u, D_V, D_V)
    loads = [
        pltpu.make_async_copy(src, dst, load.at[k])
        for k, (src, dst) in enumerate((
            (lat_in, lat_ref),
            (q_in, q_ref),
            (do_in, do_ref),
            (pos_in, pos_ref),
            (ku_in.at[:, mine_k], kuv.at[:, :D_NOPE]),
            (vu_in.at[:, mine_v], kuv.at[:, D_NOPE:]),
        ))
    ]
    for copy in loads[:4]:
        copy.start()
    for copy in loads[4:]:
        when(active, copy.start)
    mx[...] = jnp.full(mx.shape, NEG, F32)

    zbits = list(range(nb - 1, 0, -1))
    order = zbits + [0]
    masks = [
        sum(1 << b for b in some)
        for size in range(1, nb + 1)
        for some in itertools.combinations(order, size)
    ]
    zmoves = [m for m in masks if not m & 1]
    by_seq, by_core, by_y, by_both = {}, {}, {}, {}
    sub = D_ALL // nhead

    def quarter(h, s):
        return lat.at[at(h, sub, sub), at(s, rows, rows)]

    def forward(mask):
        piece = quarter(head, xor(seq, mask))
        source = piece if mask else lat_ref.at[at(head, sub, sub)]
        for to in [1] if mask else zmoves + [1]:
            by_seq[mask | to] = sems.copy(
                source, piece, on_seq(xor(seq, to)), group="lat"
            )

    def relay(mask):
        by_seq[mask].wait_recv()
        if not mask & 1:
            forward(mask)
        piece = quarter(head, xor(seq, mask))
        by_y[mask] = sems.copy(piece, piece, across, group="lat")
        by_core[mask] = sems.copy(piece, piece, other, group="lat")

    def relay_y(mask):
        by_y[mask].wait_recv()
        piece = quarter(flip(head, 1), xor(seq, mask))
        by_both[mask] = sems.copy(piece, piece, other, group="lat")

    loads[0].wait()
    pl.semaphore_wait(barrier, nseq + heads + (core - x) * (core - x))
    forward(0)
    loads[3].wait()
    for mask in range(1, nseq):
        sems.copy(pos_ref, pos.at[seq], on_seq(xor(seq, mask)), group="pos", arrive=True)
    pos_got = sems.whole(pos.at[pl.ds(0, nseq - 1)], other, "pos")
    for copy in loads[1:3]:
        copy.wait()
    for h in range(heads):
        stage[h, :D_QK, :] = q_ref[:, h * D_QK : (h + 1) * D_QK].T
        stage[h, D_QK:, :] = do_ref[:, h * D_V : (h + 1) * D_V].T
    q_got = {}
    for k in range(heads):
        q_got[k] = sems.copy(
            stage.at[pick(xor(seq, 2 * k), slot_bits)],
            qd.at[:, at(u, rows, rows)],
            swap(k),
            None if k else passive,
        )
    for copy in loads[4:]:
        when(active, copy.wait)
    kuv_got = sems.copy(kuv, kuv, other, active)
    lat[:, at(seq, rows, rows)] = lat_ref[...]
    pos[seq] = pos_ref[...]

    @pl.when(active)
    def _():
        qd[:, at(u, rows, rows)] = stage[u]

    def keys_of(s):
        here = at(s, rows, rows)
        both = nn(ut[...], lat[:D_LAT, here]).astype(BF16)
        kt[:D_NOPE, here] = both[:D_NOPE]
        vt[:, here] = both[D_NOPE:]
        kt[D_NOPE:, here] = lat[D_LAT:, here]

    down = lax.broadcasted_iota(jnp.int32, (STRIPE, rows), 0)
    per = rows // STRIPE
    lane = jnp.concatenate([lax.broadcasted_iota(jnp.int32, (1, STRIPE), 1)] * per, axis=1)

    def scores_of(s, k):
        here = at(s, rows, rows)
        keys, vals = kt[:, here], vt[:, here]
        rel = pos[s] - down
        first = pos[xor(seq, 2 * k) + core - x] - lane
        slot = pick(xor(seq, 2 * k), slot_bits)
        for t in range(per):
            part = at(slot * per + t, STRIPE, STRIPE)
            base = first[:, t * STRIPE : (t + 1) * STRIPE]
            base = jnp.concatenate([base] * per, axis=1)
            got = jnp.where(rel <= base, nn(qall[part, :], keys), NEG)
            sc[part, here] = got
            dp[part, here] = nn(dall[part, :], vals)
            top = mx[part, :]
            for c in range(rows // LANE):
                top = jnp.maximum(top, got[:, c * LANE : (c + 1) * LANE])
            mx[part, :] = top

    def turn(k):
        if k:
            q_got[k].wait_recv()
        else:
            when(passive, q_got[0].wait_recv)
        here = at(pick(xor(seq, 2 * k), slot_bits), rows, rows)
        qall[here, :] = qd[:D_QK, here].T
        dall[here, :] = qd[D_QK:, here].T

    def block_of(mask):
        by_core[mask].wait_recv()
        by_both[mask].wait_recv()
        keys_of(xor(seq, mask))

    for mask in zmoves + [1]:
        relay(mask)
    when(passive, kuv_got.wait_recv)
    ut[...] = kuv[...].T
    keys_of(seq)
    for mask in zmoves:
        relay(mask | 1)
    pos_got.wait_recv()
    early = range(heads // 2)
    for k in early:
        turn(k)
    steps = zmoves + [1] + [mask | 1 for mask in zmoves]
    behind = [0]
    for mask in steps:
        relay_y(mask)
        if len(behind) > 2:
            block = behind.pop(1)
            block_of(block)
            for k in early:
                scores_of(xor(seq, block), k)
        elif behind == [0]:
            for k in early:
                scores_of(seq, k)
        behind.append(mask)
    for block in behind[1:]:
        block_of(block)
        for k in early:
            scores_of(xor(seq, block), k)
    for k in range(heads // 2, heads):
        turn(k)
        for mask in [0] + masks:
            scores_of(xor(seq, mask), k)

    first_sent, sems.sent = sems.sent, []

    def drain(sent):
        for only in (None, active, passive):
            some = [copy for kind, copy in sent if kind is only]

            def act():
                for copy in some:
                    copy.wait_send()

            if some:
                when(only, act)

    factor = scale * LOG2E
    for t in range(nq // STRIPE):
        part = slice(t * STRIPE, (t + 1) * STRIPE)
        top = jnp.max(mx[part, :], axis=1, keepdims=True) * factor

        def sums(k, carry):
            total, weighted = carry
            here = at(k, LANE, LANE)
            e = jnp.exp2(sc[part, here] * factor - top)
            sc[part, here] = e
            return total + e, weighted + e * dp[part, here]

        zero = jnp.zeros((STRIPE, LANE), F32)
        total, weighted = loop(nk // LANE, sums, (zero, zero))
        total = jnp.sum(total, axis=1, keepdims=True)
        weighted = jnp.sum(weighted, axis=1, keepdims=True)
        inv = 1.0 / total
        sinv[part, :] = jnp.broadcast_to(inv, (STRIPE, LANE))
        sdel[part, :] = jnp.broadcast_to(weighted * inv, (STRIPE, LANE))

        def norm(k, carry):
            here = at(k, LANE, LANE)
            prob = sc[part, here] * sinv[part, :]
            sc[part, here] = prob
            pr[part, here] = prob.astype(BF16)
            return carry

        loop(nk // LANE, norm, 0)

    tile = math.gcd(nk, 512)

    def values_grad(k, carry):
        here = at(k, tile, tile)
        kvg[D_NOPE:, here] = nn(qd[D_QK:, :], pr[:, here]).astype(BF16)
        return carry

    loop(nk // tile, values_grad, 0)
    up[0] = nt(lat[:D_LAT, :], kvg[D_NOPE:, :]).astype(BF16)

    share = D_LAT // groups
    piece = share // subs

    summed, moved = {}, {}

    def source(a, i, g):
        return up.at[a, at(g * subs + i, piece, piece)]

    def place(i, s):
        return (
            at(pick(s, group_bits) * subs + i, piece, piece),
            at(pick(s, slot_bits), LANE, LANE),
        )

    def sum_start(a, i):
        for g in range(groups):
            part = at(g * subs + i, piece, piece)
            summed[a, i, g] = sems.copy(up.at[a, part], ur.at[a, part], other, passive)

    def add_up(a, i, g, ref):
        def act():
            kept = source(a, i, g)
            kept[...] = (kept[...].astype(F32) + ref[...].astype(F32)).astype(BF16)

        when(active, act)

    def sum_end(a, i):
        for g in range(groups):
            when(active, summed[a, i, g].wait_recv)
            add_up(a, i, g, ur.at[a, at(g * subs + i, piece, piece)])
        bits, slot = group_bits[::-1], 0
        for k, b in enumerate(bits):
            rest, copies = bits[k + 1 :], []
            for values in itertools.product((0, 1), repeat=len(rest)):
                to, own = flip(seq, b), seq
                for r, value in zip(rest, values):
                    to = to + (1 << r) * (value - bit(to, r))
                    own = own + (1 << r) * (value - bit(own, r))
                copy = sems.copy(
                    source(a, i, pick(to, group_bits)),
                    ug.at[a, i, slot],
                    on_seq(flip(seq, b)),
                    active,
                )
                copies.append((copy, slot, pick(own, group_bits)))
                slot += 1
            for copy, at_slot, g in copies:
                when(active, copy.wait_recv)
                add_up(a, i, g, ug.at[a, i, at_slot])

    def spread(a, i, mask, bits):
        r, c = place(i, xor(seq, mask))
        piece_at = fin.at[a, r, c]
        for b in bits:
            moved[a, i, mask | (1 << b)] = sems.copy(
                piece_at if mask else source(a, i, w),
                piece_at,
                on_seq(flip(seq, b)),
                active,
                "z" if b else "x",
            )

    def spread_z(a, i, mask):
        last = max([k for k, b in enumerate(zbits) if (mask >> b) & 1], default=-1)
        spread(a, i, mask, zbits[last + 1 :])

    def spread_x(a, i, mask):
        spread(a, i, mask, [0])

    def arrive(a, i, mask):
        when(passive if mask & 1 else active, moved[a, i, mask].wait_recv)

    def finish(a, i, mask):
        r, c = place(i, xor(seq, mask))

        def act():
            got = fin[a, r, c] if mask else source(a, i, w)[...]
            (dk_ref if a else dv_ref)[r, c] = got.astype(F32)

        when(passive if mask & 1 else active, act)

    for i in range(subs):
        sum_start(0, i)

    for t in range(nq // STRIPE):
        part = slice(t * STRIPE, (t + 1) * STRIPE)

        def scored(k, carry):
            here = at(k, LANE, LANE)
            ds[part, here] = (
                sc[part, here] * (dp[part, here] - sdel[part, :]) * scale
            ).astype(BF16)
            return carry

        loop(nk // LANE, scored, 0)

    for i in range(subs):
        sum_end(0, i)
        spread_z(0, i, 0)
        spread_x(0, i, 0)
    dqt[...] = nt(kt[...], ds[...]).astype(BF16)
    dq_in = [
        sems.copy(
            dqt.at[:, at(pick(xor(seq, 2 * k), slot_bits), rows, rows)],
            dqr.at[u],
            swap(k),
            None if k else passive,
        )
        for k in range(heads)
    ]

    @pl.when(active)
    def _():
        dqr[u] = dqt[:, at(u, rows, rows)]

    def keys_grad(k, carry):
        here = at(k, tile, tile)
        got = nn(qd[:D_QK, :], ds[:, here]).astype(BF16)
        kvg[:D_NOPE, here] = got[:D_NOPE]
        rp[:, here] = got[D_NOPE:]
        return carry

    loop(nk // tile, keys_grad, 0)

    zmasks = list(range(1, nz))[::-1] + [0]
    to_core, to_y, to_x, to_z = {}, {}, {}, {}
    mine, others = y * 2 + core, (1 - y) * 2 + core

    def fold(k):
        here = at(xor(z, k), 2 * rows, 2 * rows)
        got = nn(kuv[...], kvg[:, here]).astype(BF16)
        got = jnp.concatenate([got, rp[:, here]], axis=0)
        for h in range(nhead):
            lg[h, k] = got[h * sub : (h + 1) * sub]
        to_core[k] = [
            sems.copy(lg.at[t * 2 + 1 - core, k], rc.at[j, k], other, group="wide")
            for j, t in ((0, 1 - y), (1, y))
        ]

    def add_core(k):
        to_core[k][0].wait_recv()
        lg[others, k] = (lg[others, k].astype(F32) + rc[0, k].astype(F32)).astype(BF16)
        to_y[k] = sems.copy(lg.at[others, k], ry.at[k], across, group="wide")
        to_core[k][1].wait_recv()
        lg[mine, k] = (lg[mine, k].astype(F32) + rc[1, k].astype(F32)).astype(BF16)

    def add_y(k):
        to_y[k].wait_recv()
        lg[mine, k] = (lg[mine, k].astype(F32) + ry[k].astype(F32)).astype(BF16)
        to_x[k] = sems.copy(
            lg.at[mine, k, :, at(1 - x, rows, rows)],
            rx.at[k],
            on_seq(flip(seq, 0)),
            group="narrow",
        )

    def add_x(k):
        to_x[k].wait_recv()
        kept = lg[mine, k, :, at(x, rows, rows)].astype(F32) + rx[k].astype(F32)
        ac[k] = kept.astype(BF16)
        if k:
            to_z[k] = sems.copy(ac.at[k], rz.at[k], on_seq(xor(seq, 2 * k)), group="narrow")

    chunks = [(a, i) for a in range(2) for i in range(subs)]
    values, keys = chunks[:subs], chunks[subs:]
    near_z = [m for m in zmoves if m.bit_count() == 1]
    far_z = [m for m in zmoves if m.bit_count() > 1]

    for k in zmasks:
        fold(k)
    up[1] = nt(lat[:D_LAT, :], kvg[:D_NOPE, :]).astype(BF16)
    for i in range(subs):
        sum_start(1, i)
    for k in zmasks:
        add_core(k)
    for a, i in keys:
        sum_end(a, i)
        spread_z(a, i, 0)
        spread_x(a, i, 0)
    for chunk in chunks:
        finish(*chunk, 0)

    held = []

    def along_z(some, mask, hold=False):
        for chunk in some:
            arrive(*chunk, mask)
            spread_z(*chunk, mask)
            if hold:
                held.append((*chunk, mask))
            else:
                spread_x(*chunk, mask)
            finish(*chunk, mask)

    for mask in near_z[1:][::-1]:
        along_z(values, mask)
    drain(first_sent)
    sems.whole(lat.at[:, pl.ds(0, (nseq - 1) * rows)], other, "lat").wait_send()
    pos_got.wait_send()
    for k in zmasks[:-3]:
        add_y(k)
    for mask in near_z[1:][::-1]:
        along_z(keys, mask)
    for k in zmasks[-3:-2]:
        add_y(k)
    along_z(values, near_z[0])
    for k in zmasks[-2:-1]:
        add_y(k)
    along_z(keys, near_z[0], True)
    for k in zmasks[:1]:
        add_x(k)
    for k in zmasks[-1:]:
        add_y(k)
    for move in held:
        spread_x(*move)
    for k in zmasks[1:-1]:
        add_x(k)
    last_sent, sems.sent = sems.sent, []
    for mask in far_z:
        along_z(chunks, mask)
    add_x(0)
    total = ac[0].astype(F32)
    for k in zmasks[:-1]:
        to_z[k].wait_recv()
        total = total + rz[k].astype(F32)
    fl[head] = total.astype(BF16)
    first = sems.copy(fl.at[head], fl.at[head], across, group="narrow")
    second = sems.copy(fl.at[head], fl.at[head], other, group="narrow")
    drain(last_sent)
    when(active, sems.whole(fin.at[:, : D_LAT * (nz - 1) // nz], other, "z").wait_send)
    sems.whole(lg.at[: nhead - 1], other, "wide").wait_send()
    for copy in dq_in[1:]:
        copy.wait_recv()
    when(passive, dq_in[0].wait_recv)
    for h in range(heads):
        dq_ref[:, h * D_QK : (h + 1) * D_QK] = dqr[h].T
    first.wait_recv()
    third = sems.copy(fl.at[others], fl.at[others], other, group="narrow")
    for mask in [0] + zmoves:
        for chunk in chunks:
            arrive(*chunk, mask | 1)
            finish(*chunk, mask | 1)
    second.wait_recv()
    third.wait_recv()
    for h in range(nhead):
        dl_ref[h * sub : (h + 1) * sub, :] = fl[h].astype(F32)
    assert (sems.sends, sems.recvs) == (send.shape[0], recv.shape[0])
    drain(sems.sent)
    when(active, sems.whole(fin, other, "x").wait_send)
    sems.whole(lat.at[: 2 * sub, pl.ds(0, (nz + 1) * rows)], other, "narrow").wait_send()


def store(*refs):
    sems = refs[8]
    copies = [pltpu.make_async_copy(refs[k], refs[4 + k], sems.at[k]) for k in range(4)]
    for copy in copies:
        copy.start()
    for copy in copies:
        copy.wait()


def make_shards(nseq, nhead):
    def shards(queries, latents, key_up, value_up, out_grad, positions):
        rows, heads = latents.shape[0], key_up.shape[1] // D_NOPE
        nq, nk = heads * rows, nseq * rows
        nz, groups = nseq // 2, nseq // (2 * heads)
        subs = 2
        share = D_LAT // groups
        sub = D_ALL // nhead
        cols = key_up.shape[1]
        sums = 2 * subs * (2 * groups - 1)
        sends = 2 * heads + 1 + sums + 6
        copies = (nseq - 1) * 4 + 1 + 2 * heads + 1
        copies += sums + 2 * subs * (nseq - 1) + 5 * nz + 2
        vmem = pl.BlockSpec(memory_space=pltpu.VMEM)
        body = lambda *refs: kernel(nseq, nhead, subs, *refs)
        moved = [
            (queries.shape, BF16),
            ((D_ALL, rows), BF16),
            (out_grad.shape, BF16),
            ((1, rows), jnp.int32),
        ]
        scratch = [
            ((heads, D_QK + D_V, rows), BF16),
            ((D_QK + D_V, nq), BF16),
            ((nq, D_QK), BF16),
            ((nq, D_V), BF16),
            ((D_ALL, nk), BF16),
            ((nseq, 1, rows), jnp.int32),
            ((D_QK, nk), BF16),
            ((D_V, nk), BF16),
            ((D_LAT, D_NOPE + D_V), BF16),
            ((D_NOPE + D_V, D_LAT), BF16),
            ((nq, nk), F32),
            ((nq, nk), F32),
            ((nq, LANE), F32),
            ((nq, LANE), F32),
            ((nq, LANE), F32),
            ((nq, nk), BF16),
            ((nq, nk), BF16),
            ((D_NOPE + D_V, nk), BF16),
            ((D_ROPE, nk), BF16),
            ((2, D_LAT, LANE), BF16),
            ((2, D_LAT, LANE), BF16),
            ((2, subs, max(groups - 1, 1), share // subs, LANE), BF16),
            ((2, D_LAT, cols), BF16),
            ((nhead, nz, sub, 2 * rows), BF16),
            ((nhead // 2, nz, sub, 2 * rows), BF16),
            ((nz, sub, 2 * rows), BF16),
            ((nz, sub, rows), BF16),
            ((nz, sub, rows), BF16),
            ((nz, sub, rows), BF16),
            ((nhead, sub, rows), BF16),
            ((D_QK, nq), BF16),
            ((heads, D_QK, rows), BF16),
        ]
        limit = 8 * 1024 * 1024
        for shape, dtype in moved + scratch:
            padded = (-(-shape[-1] // LANE) * LANE) * (-(-shape[-2] // 16) * 16)
            limit += math.prod(shape[:-2]) * padded * jnp.dtype(dtype).itemsize
        dq, dl, dk, dv = pl.pallas_call(
            body,
            out_shape=(
                jax.ShapeDtypeStruct(queries.shape, BF16),
                jax.ShapeDtypeStruct((D_ALL, rows), F32),
                jax.ShapeDtypeStruct(key_up.shape, F32),
                jax.ShapeDtypeStruct(value_up.shape, F32),
            ),
            in_specs=[pl.BlockSpec(memory_space=pltpu.HBM)] * 6,
            out_specs=(vmem,) * 4,
            scratch_shapes=[pltpu.VMEM(shape, dtype) for shape, dtype in moved]
            + [pltpu.SemaphoreType.DMA((6,))]
            + [pltpu.VMEM(shape, dtype) for shape, dtype in scratch]
            + [pltpu.SemaphoreType.DMA((sends,)), pltpu.SemaphoreType.DMA((copies,))],
            compiler_params=pltpu.CompilerParams(
                collective_id=0, has_side_effects=True, vmem_limit_bytes=min(limit, 60 * 1024 * 1024)
            ),
        )(*[
            pltpu.with_memory_space_constraint(a, pltpu.HBM)
            for a in (queries, latents.T, key_up, value_up, out_grad, positions[None, :])
        ])
        done = (dq, dl, dk, dv)
        dq, dl, dk, dv = pl.pallas_call(
            store,
            out_shape=[jax.ShapeDtypeStruct(a.shape, a.dtype) for a in done],
            in_specs=[vmem] * 4,
            out_specs=[pl.BlockSpec(memory_space=pltpu.HBM)] * 4,
            scratch_shapes=[pltpu.SemaphoreType.DMA((4,))],
            compiler_params=pltpu.CompilerParams(vmem_limit_bytes=1024 * 1024),
        )(*done)
        return dq, dl.T, dk, dv

    return shards


def solution(mesh):
    in_specs = (
        P("seq", "head"),
        P("seq", None),
        P(None, "head"),
        P(None, "head"),
        P("seq", "head"),
        P("seq"),
    )
    out_specs = (P("seq", "head"), P("seq", None), P(None, "head"), P(None, "head"))
    shards = make_shards(mesh.shape["seq"], mesh.shape["head"])
    return jax.shard_map(shards, mesh=mesh, in_specs=in_specs, out_specs=out_specs, check_vma=False)
```

```python
import itertools
import math

import jax
import jax.numpy as jnp
from jax import lax
from jax.experimental import pallas as pl
from jax.experimental.pallas import tpu as pltpu
from jax.sharding import PartitionSpec as P

D_LAT = 512
D_ROPE = 64
D_NOPE = 128
D_V = 128
D_QK = D_NOPE + D_ROPE
D_ALL = D_LAT + D_ROPE
LANE = 128
STRIPE = 128
NEG = -1e30
LOG2E = 1.4426950408889634
MESH = pl.DeviceIdType.MESH
F32 = jnp.float32
BF16 = jnp.bfloat16


def bit(index, b):
    return (index // (1 << b)) % 2


def flip(index, b):
    return index + (1 << b) * (1 - 2 * bit(index, b))


def xor(index, mask):
    b = 0
    while mask >> b:
        if (mask >> b) & 1:
            index = flip(index, b)
        b += 1
    return index


def pick(index, bits):
    out = 0
    for k, b in enumerate(bits):
        out = out + (1 << k) * bit(index, b)
    return out


def put(index, bits, value):
    for k, b in enumerate(bits):
        index = index + (1 << b) * (((value >> k) & 1) - bit(index, b))
    return index


def nn(a, b):
    return lax.dot_general(a, b, (((1,), (0,)), ((), ())), preferred_element_type=F32)


def nt(a, b):
    return lax.dot_general(a, b, (((1,), (1,)), ((), ())), preferred_element_type=F32)


def loop(n, body, init):
    if n <= 8:
        for t in range(n):
            init = body(t, init)
        return init
    return lax.fori_loop(0, n, body, init)


def when(only, act):
    if only is None:
        act()
    else:
        pl.when(only)(act)


class Sems:
    def __init__(self, send, recv):
        self.send, self.recv = send, recv
        self.sends, self.recvs, self.shared = 0, 0, {}
        self.sent = []

    def slots(self, group, arrive):
        if ("send", group) not in self.shared:
            if group is not None:
                self.shared["send", group] = self.sends
            out = self.sends
            self.sends += 1
        else:
            out = self.shared["send", group]
        if not arrive:
            into = self.recvs
            self.recvs += 1
        else:
            into = self.shared.setdefault(("recv", group), self.recvs)
            self.recvs = max(self.recvs, into + 1)
        return self.send.at[out], self.recv.at[into]

    def make(self, src, dst, device, group=None, arrive=False):
        send, recv = self.slots(group, arrive)
        return pltpu.make_async_remote_copy(
            src_ref=src,
            dst_ref=dst,
            send_sem=send,
            recv_sem=recv,
            device_id=device,
            device_id_type=MESH,
        )

    def copy(self, src, dst, device, only=None, group=None, arrive=False):
        copy = self.make(src, dst, device, group, arrive)
        when(only, copy.start)
        if group is None:
            self.sent.append((only, copy))
        return copy

    def whole(self, ref, device, group):
        send = self.send.at[self.shared["send", group]]
        recv = self.recv.at[self.shared.get(("recv", group), 0)]
        return pltpu.make_async_remote_copy(
            src_ref=ref,
            dst_ref=ref,
            send_sem=send,
            recv_sem=recv,
            device_id=device,
            device_id_type=MESH,
        )


def kernel(
    nseq, nhead, subs,
    q_in, lat_in, ku_in, vu_in, do_in, pos_in,
    dq_ref, dl_ref, dk_ref, dv_ref,
    q_ref, lat_ref, do_ref, pos_ref, load,
    stage, qd, qall, dall, lat, pos, kt, vt, kuv, ut, sc, dp, mx, sinv, sdel,
    pr, ds, kvg, rp, up, ur, ug, fin, lg, rc, ry, rx, ac, rz, fl, dqt, dqr,
    send, recv,
):
    seq, head = lax.axis_index("seq"), lax.axis_index("head")
    rows = lat_in.shape[1]
    heads = ku_in.shape[1] // D_NOPE
    nq, nk = heads * rows, nseq * rows
    nb = nseq.bit_length() - 1
    hb = heads.bit_length() - 1
    slot_bits = list(range(1, 1 + hb))
    group_bits = list(range(1 + hb, nb))
    groups = 1 << len(group_bits)
    nz = nseq // 2
    scale = 1.0 / math.sqrt(D_QK)
    sems = Sems(send, recv)
    u, w = pick(seq, slot_bits), pick(seq, group_bits)
    x, z = bit(seq, 0), seq // 2
    core, y = bit(head, 0), bit(head, 1)
    active, passive = core == x, core != x

    def on_seq(s):
        return (s, head)

    def on_head(h):
        return (seq, h)

    other = on_head(flip(head, 0))
    across = on_head(flip(head, 1))

    barrier = pltpu.get_barrier_semaphore()
    for mask in range(1, nseq):
        pl.semaphore_signal(barrier, inc=1, device_id=on_seq(xor(seq, mask)), device_id_type=MESH)
    for device in (other, across):
        pl.semaphore_signal(barrier, inc=1, device_id=device, device_id_type=MESH)

    def swap(k):
        return (xor(seq, 2 * k) + core - x, head + x - core)

    def greet(k):
        pl.semaphore_signal(barrier, inc=1, device_id=swap(k), device_id_type=MESH)

    for k in range(1, heads):
        greet(k)
    when(passive, lambda: greet(0))

    def at(start, size, step):
        return pl.ds(pl.multiple_of(start * step, step), size)

    mine_k, mine_v = at(u, D_NOPE, D_NOPE), at(u, D_V, D_V)
    loads = [
        pltpu.make_async_copy(src, dst, load.at[k])
        for k, (src, dst) in enumerate((
            (lat_in, lat_ref),
            (q_in, q_ref),
            (do_in, do_ref),
            (pos_in, pos_ref),
            (ku_in.at[:, mine_k], kuv.at[:, :D_NOPE]),
            (vu_in.at[:, mine_v], kuv.at[:, D_NOPE:]),
        ))
    ]
    for copy in loads[:4]:
        copy.start()
    for copy in loads[4:]:
        when(active, copy.start)
    mx[...] = jnp.full(mx.shape, NEG, F32)

    zbits = list(range(nb - 1, 0, -1))
    order = zbits + [0]
    masks = [
        sum(1 << b for b in some)
        for size in range(1, nb + 1)
        for some in itertools.combinations(order, size)
    ]
    zmoves = [m for m in masks if not m & 1]
    by_seq, by_core, by_y, by_both = {}, {}, {}, {}
    sub = D_ALL // nhead

    def quarter(h, s):
        return lat.at[at(h, sub, sub), at(s, rows, rows)]

    def forward(mask):
        piece = quarter(head, xor(seq, mask))
        source = piece if mask else lat_ref.at[at(head, sub, sub)]
        for to in [1] if mask else zmoves + [1]:
            by_seq[mask | to] = sems.copy(
                source, piece, on_seq(xor(seq, to)), group="lat"
            )

    def relay(mask):
        by_seq[mask].wait_recv()
        if not mask & 1:
            forward(mask)
        piece = quarter(head, xor(seq, mask))
        by_y[mask] = sems.copy(piece, piece, across, group="lat")
        by_core[mask] = sems.copy(piece, piece, other, group="lat")

    def relay_y(mask):
        by_y[mask].wait_recv()
        piece = quarter(flip(head, 1), xor(seq, mask))
        by_both[mask] = sems.copy(piece, piece, other, group="lat")

    loads[0].wait()
    pl.semaphore_wait(barrier, nseq + heads + (core - x) * (core - x))
    forward(0)
    loads[3].wait()
    for mask in range(1, nseq):
        sems.copy(pos_ref, pos.at[seq], on_seq(xor(seq, mask)), group="pos", arrive=True)
    pos_got = sems.whole(pos.at[pl.ds(0, nseq - 1)], other, "pos")
    for copy in loads[1:3]:
        copy.wait()
    for h in range(heads):
        stage[h, :D_QK, :] = q_ref[:, h * D_QK : (h + 1) * D_QK].T
        stage[h, D_QK:, :] = do_ref[:, h * D_V : (h + 1) * D_V].T
    q_got = {}
    for k in range(heads):
        q_got[k] = sems.copy(
            stage.at[pick(xor(seq, 2 * k), slot_bits)],
            qd.at[:, at(u, rows, rows)],
            swap(k),
            None if k else passive,
        )
    for copy in loads[4:]:
        when(active, copy.wait)
    kuv_got = sems.copy(kuv, kuv, other, active)
    lat[:, at(seq, rows, rows)] = lat_ref[...]
    pos[seq] = pos_ref[...]

    @pl.when(active)
    def _():
        qd[:, at(u, rows, rows)] = stage[u]

    def keys_of(s):
        here = at(s, rows, rows)
        both = nn(ut[...], lat[:D_LAT, here]).astype(BF16)
        kt[:D_NOPE, here] = both[:D_NOPE]
        vt[:, here] = both[D_NOPE:]
        kt[D_NOPE:, here] = lat[D_LAT:, here]

    down = lax.broadcasted_iota(jnp.int32, (STRIPE, rows), 0)
    per = rows // STRIPE
    lane = jnp.concatenate([lax.broadcasted_iota(jnp.int32, (1, STRIPE), 1)] * per, axis=1)

    def scores_of(s, k):
        here = at(s, rows, rows)
        keys, vals = kt[:, here], vt[:, here]
        rel = pos[s] - down
        first = pos[xor(seq, 2 * k) + core - x] - lane
        slot = pick(xor(seq, 2 * k), slot_bits)
        for t in range(per):
            part = at(slot * per + t, STRIPE, STRIPE)
            base = first[:, t * STRIPE : (t + 1) * STRIPE]
            base = jnp.concatenate([base] * per, axis=1)
            got = jnp.where(rel <= base, nn(qall[part, :], keys), NEG)
            sc[part, here] = got
            dp[part, here] = nn(dall[part, :], vals)
            top = mx[part, :]
            for c in range(rows // LANE):
                top = jnp.maximum(top, got[:, c * LANE : (c + 1) * LANE])
            mx[part, :] = top

    def scores_pair(p, k):
        here = slice(2 * p * rows, 2 * (p + 1) * rows)
        keys, vals = kt[:, here], vt[:, here]
        rel = jnp.concatenate([pos[2 * p] - down, pos[2 * p + 1] - down], axis=1)
        first = pos[xor(seq, 2 * k) + core - x] - lane
        slot = pick(xor(seq, 2 * k), slot_bits)
        for t in range(per):
            part = at(slot * per + t, STRIPE, STRIPE)
            base = first[:, t * STRIPE : (t + 1) * STRIPE]
            base = jnp.concatenate([base] * (2 * per), axis=1)
            got = jnp.where(rel <= base, nn(qall[part, :], keys), NEG)
            sc[part, here] = got
            dp[part, here] = nn(dall[part, :], vals)
            top = mx[part, :]
            for c in range(2 * rows // LANE):
                top = jnp.maximum(top, got[:, c * LANE : (c + 1) * LANE])
            mx[part, :] = top

    def turn(k):
        if k:
            q_got[k].wait_recv()
        else:
            when(passive, q_got[0].wait_recv)
        here = at(pick(xor(seq, 2 * k), slot_bits), rows, rows)
        qall[here, :] = qd[:D_QK, here].T
        dall[here, :] = qd[D_QK:, here].T

    def block_of(mask):
        by_core[mask].wait_recv()
        by_both[mask].wait_recv()
        keys_of(xor(seq, mask))

    for mask in zmoves + [1]:
        relay(mask)
    when(passive, kuv_got.wait_recv)
    ut[...] = kuv[...].T
    keys_of(seq)
    early = range(heads // 2)
    relay(zmoves[0] | 1)
    turn(0)
    for mask in zmoves[1:]:
        relay(mask | 1)
    pos_got.wait_recv()
    turn(1)
    steps = zmoves + [1] + [mask | 1 for mask in zmoves]
    behind = [0]
    for mask in steps:
        relay_y(mask)
        if len(behind) > 2:
            block = behind.pop(1)
            block_of(block)
            for k in early:
                scores_of(xor(seq, block), k)
        elif behind == [0]:
            for k in early:
                scores_of(seq, k)
        behind.append(mask)
    for block in behind[1:]:
        block_of(block)
        for k in early:
            scores_of(xor(seq, block), k)
    for k in range(heads // 2, heads):
        turn(k)
        for p in range(nz):
            scores_pair(p, k)

    first_sent, sems.sent = sems.sent, []

    def drain(sent):
        for only in (None, active, passive):
            some = [copy for kind, copy in sent if kind is only]

            def act():
                for copy in some:
                    copy.wait_send()

            if some:
                when(only, act)

    factor = scale * LOG2E
    for t in range(nq // STRIPE):
        part = slice(t * STRIPE, (t + 1) * STRIPE)
        top = jnp.max(mx[part, :], axis=1, keepdims=True) * factor

        def sums(k, carry):
            total, weighted = carry
            here = at(k, LANE, LANE)
            e = jnp.exp2(sc[part, here] * factor - top)
            sc[part, here] = e
            return total + e, weighted + e * dp[part, here]

        zero = jnp.zeros((STRIPE, LANE), F32)
        total, weighted = loop(nk // LANE, sums, (zero, zero))
        total = jnp.sum(total, axis=1, keepdims=True)
        weighted = jnp.sum(weighted, axis=1, keepdims=True)
        inv = 1.0 / total
        sinv[part, :] = jnp.broadcast_to(inv, (STRIPE, LANE))
        sdel[part, :] = jnp.broadcast_to(weighted * inv, (STRIPE, LANE))

        def norm(k, carry):
            here = at(k, LANE, LANE)
            prob = sc[part, here] * sinv[part, :]
            sc[part, here] = prob
            pr[part, here] = prob.astype(BF16)
            return carry

        loop(nk // LANE, norm, 0)

    tile = math.gcd(nk, 512)

    def values_grad(k, carry):
        here = at(k, tile, tile)
        kvg[D_NOPE:, here] = nn(qd[D_QK:, :], pr[:, here]).astype(BF16)
        return carry

    loop(nk // tile, values_grad, 0)
    up[0] = nt(lat[:D_LAT, :], kvg[D_NOPE:, :]).astype(BF16)

    share = D_LAT // groups
    piece = share // subs

    summed, moved = {}, {}

    def source(a, i, g):
        return up.at[a, at(g * subs + i, piece, piece)]

    def place(i, s):
        return (
            at(pick(s, group_bits) * subs + i, piece, piece),
            at(pick(s, slot_bits), LANE, LANE),
        )

    def sum_start(a, i):
        for g in range(groups):
            part = at(g * subs + i, piece, piece)
            summed[a, i, g] = sems.copy(up.at[a, part], ur.at[a, part], other, passive)

    def add_up(a, i, g, ref):
        def act():
            kept = source(a, i, g)
            kept[...] = (kept[...].astype(F32) + ref[...].astype(F32)).astype(BF16)

        when(active, act)

    def sum_end(a, i):
        for g in range(groups):
            when(active, summed[a, i, g].wait_recv)
            add_up(a, i, g, ur.at[a, at(g * subs + i, piece, piece)])
        bits, slot = group_bits[::-1], 0
        for k, b in enumerate(bits):
            rest, copies = bits[k + 1 :], []
            for values in itertools.product((0, 1), repeat=len(rest)):
                to, own = flip(seq, b), seq
                for r, value in zip(rest, values):
                    to = to + (1 << r) * (value - bit(to, r))
                    own = own + (1 << r) * (value - bit(own, r))
                copy = sems.copy(
                    source(a, i, pick(to, group_bits)),
                    ug.at[a, i, slot],
                    on_seq(flip(seq, b)),
                    active,
                )
                copies.append((copy, slot, pick(own, group_bits)))
                slot += 1
            for copy, at_slot, g in copies:
                when(active, copy.wait_recv)
                add_up(a, i, g, ug.at[a, i, at_slot])

    def spread(a, i, mask, bits):
        r, c = place(i, xor(seq, mask))
        piece_at = fin.at[a, r, c]
        for b in bits:
            moved[a, i, mask | (1 << b)] = sems.copy(
                piece_at if mask else source(a, i, w),
                piece_at,
                on_seq(flip(seq, b)),
                active,
                "z" if b else "x",
            )

    def spread_z(a, i, mask):
        last = max([k for k, b in enumerate(zbits) if (mask >> b) & 1], default=-1)
        spread(a, i, mask, zbits[last + 1 :])

    def spread_x(a, i, mask):
        spread(a, i, mask, [0])

    def arrive(a, i, mask):
        when(passive if mask & 1 else active, moved[a, i, mask].wait_recv)

    def finish(a, i, mask):
        r, c = place(i, xor(seq, mask))

        def act():
            got = fin[a, r, c] if mask else source(a, i, w)[...]
            (dk_ref if a else dv_ref)[r, c] = got.astype(F32)

        when(passive if mask & 1 else active, act)

    for i in range(subs):
        sum_start(0, i)

    for t in range(nq // STRIPE):
        part = slice(t * STRIPE, (t + 1) * STRIPE)

        def scored(k, carry):
            here = at(k, LANE, LANE)
            ds[part, here] = (
                sc[part, here] * (dp[part, here] - sdel[part, :]) * scale
            ).astype(BF16)
            return carry

        loop(nk // LANE, scored, 0)

    for i in range(subs):
        sum_end(0, i)
        spread_z(0, i, 0)
        spread_x(0, i, 0)
    dqt[...] = nt(kt[...], ds[...]).astype(BF16)
    dq_in = [
        sems.copy(
            dqt.at[:, at(pick(xor(seq, 2 * k), slot_bits), rows, rows)],
            dqr.at[u],
            swap(k),
            None if k else passive,
        )
        for k in range(heads)
    ]

    @pl.when(active)
    def _():
        dqr[u] = dqt[:, at(u, rows, rows)]

    def keys_grad(k, carry):
        here = at(k, tile, tile)
        got = nn(qd[:D_QK, :], ds[:, here]).astype(BF16)
        kvg[:D_NOPE, here] = got[:D_NOPE]
        rp[:, here] = got[D_NOPE:]
        return carry

    loop(nk // tile, keys_grad, 0)

    zmasks = list(range(1, nz))[::-1] + [0]
    to_core, to_y, to_x, to_z = {}, {}, {}, {}
    mine, others = y * 2 + core, (1 - y) * 2 + core

    def fold(k):
        here = at(xor(z, k), 2 * rows, 2 * rows)
        got = nn(kuv[...], kvg[:, here]).astype(BF16)
        got = jnp.concatenate([got, rp[:, here]], axis=0)
        for h in range(nhead):
            lg[h, k] = got[h * sub : (h + 1) * sub]

    def share_fold(k):
        to_core[k] = [
            sems.copy(lg.at[t * 2 + 1 - core, k], rc.at[j, k], other, group="wide")
            for j, t in ((0, 1 - y), (1, y))
        ]

    def add_core(k):
        to_core[k][0].wait_recv()
        lg[others, k] = (lg[others, k].astype(F32) + rc[0, k].astype(F32)).astype(BF16)
        to_y[k] = sems.copy(lg.at[others, k], ry.at[k], across, group="wide")
        to_core[k][1].wait_recv()
        lg[mine, k] = (lg[mine, k].astype(F32) + rc[1, k].astype(F32)).astype(BF16)

    def add_y(k):
        to_y[k].wait_recv()
        lg[mine, k] = (lg[mine, k].astype(F32) + ry[k].astype(F32)).astype(BF16)
        to_x[k] = sems.copy(
            lg.at[mine, k, :, at(1 - x, rows, rows)],
            rx.at[k],
            on_seq(flip(seq, 0)),
            group="narrow",
        )

    def add_x(k):
        to_x[k].wait_recv()
        kept = lg[mine, k, :, at(x, rows, rows)].astype(F32) + rx[k].astype(F32)
        ac[k] = kept.astype(BF16)
        if k:
            to_z[k] = sems.copy(ac.at[k], rz.at[k], on_seq(xor(seq, 2 * k)), group="narrow")

    chunks = [(a, i) for a in range(2) for i in range(subs)]
    values, keys = chunks[:subs], chunks[subs:]
    near_z = [m for m in zmoves if m.bit_count() == 1]
    far_z = [m for m in zmoves if m.bit_count() > 1]

    for k in zmasks:
        fold(k)
    for k in zmasks:
        share_fold(k)
    up[1] = nt(lat[:D_LAT, :], kvg[:D_NOPE, :]).astype(BF16)
    for i in range(subs):
        sum_start(1, i)
    for k in zmasks:
        add_core(k)
    for a, i in keys:
        sum_end(a, i)
        spread_z(a, i, 0)
        spread_x(a, i, 0)
    for chunk in chunks:
        finish(*chunk, 0)

    held = []

    def along_z(some, mask, hold=False):
        for chunk in some:
            arrive(*chunk, mask)
            spread_z(*chunk, mask)
            if hold:
                held.append((*chunk, mask))
            else:
                spread_x(*chunk, mask)
            finish(*chunk, mask)

    for mask in near_z[1:][::-1]:
        along_z(values, mask)
    drain(first_sent)
    sems.whole(lat.at[:, pl.ds(0, (nseq - 1) * rows)], other, "lat").wait_send()
    pos_got.wait_send()
    for k in zmasks[:-1]:
        add_y(k)
    for mask in near_z[1:][::-1]:
        along_z(keys, mask)
    for k in zmasks[:-3]:
        add_x(k)
    along_z(values, near_z[0])
    for k in zmasks[-1:]:
        add_y(k)
    for k in zmasks[-3:-2]:
        add_x(k)
    along_z(keys, near_z[0], True)
    for k in zmasks[-2:-1]:
        add_x(k)
    for move in held:
        spread_x(*move)
    last_sent, sems.sent = sems.sent, []
    for mask in far_z:
        along_z(chunks, mask)
    add_x(0)
    total = ac[0].astype(F32)
    for k in zmasks[:-1]:
        to_z[k].wait_recv()
        total = total + rz[k].astype(F32)
    fl[head] = total.astype(BF16)
    first = sems.copy(fl.at[head], fl.at[head], across, group="narrow")
    second = sems.copy(fl.at[head], fl.at[head], other, group="narrow")
    drain(last_sent)
    when(active, sems.whole(fin.at[:, : D_LAT * (nz - 1) // nz], other, "z").wait_send)
    sems.whole(lg.at[: nhead - 1], other, "wide").wait_send()
    for copy in dq_in[1:]:
        copy.wait_recv()
    when(passive, dq_in[0].wait_recv)
    for h in range(heads):
        dq_ref[:, h * D_QK : (h + 1) * D_QK] = dqr[h].T
    first.wait_recv()
    third = sems.copy(fl.at[others], fl.at[others], other, group="narrow")
    for mask in [0] + zmoves:
        for chunk in chunks:
            arrive(*chunk, mask | 1)
            finish(*chunk, mask | 1)
    second.wait_recv()
    third.wait_recv()
    for h in range(nhead):
        dl_ref[h * sub : (h + 1) * sub, :] = fl[h].astype(F32)
    assert (sems.sends, sems.recvs) == (send.shape[0], recv.shape[0])
    drain(sems.sent)
    when(active, sems.whole(fin, other, "x").wait_send)
    sems.whole(lat.at[: 2 * sub, pl.ds(0, (nz + 1) * rows)], other, "narrow").wait_send()


def store(*refs):
    sems = refs[8]
    copies = [pltpu.make_async_copy(refs[k], refs[4 + k], sems.at[k]) for k in range(4)]
    for copy in copies:
        copy.start()
    for copy in copies:
        copy.wait()


def make_shards(nseq, nhead):
    def shards(queries, latents, key_up, value_up, out_grad, positions):
        rows, heads = latents.shape[0], key_up.shape[1] // D_NOPE
        nq, nk = heads * rows, nseq * rows
        nz, groups = nseq // 2, nseq // (2 * heads)
        subs = 2
        share = D_LAT // groups
        sub = D_ALL // nhead
        cols = key_up.shape[1]
        sums = 2 * subs * (2 * groups - 1)
        sends = 2 * heads + 1 + sums + 6
        copies = (nseq - 1) * 4 + 1 + 2 * heads + 1
        copies += sums + 2 * subs * (nseq - 1) + 5 * nz + 2
        vmem = pl.BlockSpec(memory_space=pltpu.VMEM)
        body = lambda *refs: kernel(nseq, nhead, subs, *refs)
        moved = [
            (queries.shape, BF16),
            ((D_ALL, rows), BF16),
            (out_grad.shape, BF16),
            ((1, rows), jnp.int32),
        ]
        scratch = [
            ((heads, D_QK + D_V, rows), BF16),
            ((D_QK + D_V, nq), BF16),
            ((nq, D_QK), BF16),
            ((nq, D_V), BF16),
            ((D_ALL, nk), BF16),
            ((nseq, 1, rows), jnp.int32),
            ((D_QK, nk), BF16),
            ((D_V, nk), BF16),
            ((D_LAT, D_NOPE + D_V), BF16),
            ((D_NOPE + D_V, D_LAT), BF16),
            ((nq, nk), F32),
            ((nq, nk), F32),
            ((nq, LANE), F32),
            ((nq, LANE), F32),
            ((nq, LANE), F32),
            ((nq, nk), BF16),
            ((nq, nk), BF16),
            ((D_NOPE + D_V, nk), BF16),
            ((D_ROPE, nk), BF16),
            ((2, D_LAT, LANE), BF16),
            ((2, D_LAT, LANE), BF16),
            ((2, subs, max(groups - 1, 1), share // subs, LANE), BF16),
            ((2, D_LAT, cols), BF16),
            ((nhead, nz, sub, 2 * rows), BF16),
            ((nhead // 2, nz, sub, 2 * rows), BF16),
            ((nz, sub, 2 * rows), BF16),
            ((nz, sub, rows), BF16),
            ((nz, sub, rows), BF16),
            ((nz, sub, rows), BF16),
            ((nhead, sub, rows), BF16),
            ((D_QK, nq), BF16),
            ((heads, D_QK, rows), BF16),
        ]
        limit = 8 * 1024 * 1024
        for shape, dtype in moved + scratch:
            padded = (-(-shape[-1] // LANE) * LANE) * (-(-shape[-2] // 16) * 16)
            limit += math.prod(shape[:-2]) * padded * jnp.dtype(dtype).itemsize
        dq, dl, dk, dv = pl.pallas_call(
            body,
            out_shape=(
                jax.ShapeDtypeStruct(queries.shape, BF16),
                jax.ShapeDtypeStruct((D_ALL, rows), F32),
                jax.ShapeDtypeStruct(key_up.shape, F32),
                jax.ShapeDtypeStruct(value_up.shape, F32),
            ),
            in_specs=[pl.BlockSpec(memory_space=pltpu.HBM)] * 6,
            out_specs=(vmem,) * 4,
            scratch_shapes=[pltpu.VMEM(shape, dtype) for shape, dtype in moved]
            + [pltpu.SemaphoreType.DMA((6,))]
            + [pltpu.VMEM(shape, dtype) for shape, dtype in scratch]
            + [pltpu.SemaphoreType.DMA((sends,)), pltpu.SemaphoreType.DMA((copies,))],
            compiler_params=pltpu.CompilerParams(
                collective_id=0, has_side_effects=True, vmem_limit_bytes=min(limit, 60 * 1024 * 1024)
            ),
        )(*[
            pltpu.with_memory_space_constraint(a, pltpu.HBM)
            for a in (queries, latents.T, key_up, value_up, out_grad, positions[None, :])
        ])
        done = (dq, dl, dk, dv)
        dq, dl, dk, dv = pl.pallas_call(
            store,
            out_shape=[jax.ShapeDtypeStruct(a.shape, a.dtype) for a in done],
            in_specs=[vmem] * 4,
            out_specs=[pl.BlockSpec(memory_space=pltpu.HBM)] * 4,
            scratch_shapes=[pltpu.SemaphoreType.DMA((4,))],
            compiler_params=pltpu.CompilerParams(vmem_limit_bytes=1024 * 1024),
        )(*done)
        return dq, dl.T, dk, dv

    return shards


def solution(mesh):
    in_specs = (
        P("seq", "head"),
        P("seq", None),
        P(None, "head"),
        P(None, "head"),
        P("seq", "head"),
        P("seq"),
    )
    out_specs = (P("seq", "head"), P("seq", None), P(None, "head"), P(None, "head"))
    shards = make_shards(mesh.shape["seq"], mesh.shape["head"])
    return jax.shard_map(shards, mesh=mesh, in_specs=in_specs, out_specs=out_specs, check_vma=False)
```

```python
import itertools
import math

import jax
import jax.numpy as jnp
from jax import lax
from jax.experimental import pallas as pl
from jax.experimental.pallas import tpu as pltpu
from jax.sharding import PartitionSpec as P

D_LAT = 512
D_ROPE = 64
D_NOPE = 128
D_V = 128
D_QK = D_NOPE + D_ROPE
D_ALL = D_LAT + D_ROPE
LANE = 128
STRIPE = 128
NEG = -1e30
LOG2E = 1.4426950408889634
MESH = pl.DeviceIdType.MESH
F32 = jnp.float32
BF16 = jnp.bfloat16


def bit(index, b):
    return (index // (1 << b)) % 2


def flip(index, b):
    return index + (1 << b) * (1 - 2 * bit(index, b))


def xor(index, mask):
    b = 0
    while mask >> b:
        if (mask >> b) & 1:
            index = flip(index, b)
        b += 1
    return index


def pick(index, bits):
    out = 0
    for k, b in enumerate(bits):
        out = out + (1 << k) * bit(index, b)
    return out


def put(index, bits, value):
    for k, b in enumerate(bits):
        index = index + (1 << b) * (((value >> k) & 1) - bit(index, b))
    return index


def nn(a, b):
    return lax.dot_general(a, b, (((1,), (0,)), ((), ())), preferred_element_type=F32)


def nt(a, b):
    return lax.dot_general(a, b, (((1,), (1,)), ((), ())), preferred_element_type=F32)


def loop(n, body, init):
    if n <= 8:
        for t in range(n):
            init = body(t, init)
        return init
    return lax.fori_loop(0, n, body, init)


def when(only, act):
    if only is None:
        act()
    else:
        pl.when(only)(act)


class Sems:
    def __init__(self, send, recv):
        self.send, self.recv = send, recv
        self.sends, self.recvs, self.shared = 0, 0, {}
        self.sent = []

    def slots(self, group, arrive):
        if ("send", group) not in self.shared:
            if group is not None:
                self.shared["send", group] = self.sends
            out = self.sends
            self.sends += 1
        else:
            out = self.shared["send", group]
        if not arrive:
            into = self.recvs
            self.recvs += 1
        else:
            into = self.shared.setdefault(("recv", group), self.recvs)
            self.recvs = max(self.recvs, into + 1)
        return self.send.at[out], self.recv.at[into]

    def make(self, src, dst, device, group=None, arrive=False):
        send, recv = self.slots(group, arrive)
        return pltpu.make_async_remote_copy(
            src_ref=src,
            dst_ref=dst,
            send_sem=send,
            recv_sem=recv,
            device_id=device,
            device_id_type=MESH,
        )

    def copy(self, src, dst, device, only=None, group=None, arrive=False):
        copy = self.make(src, dst, device, group, arrive)
        when(only, copy.start)
        if group is None:
            self.sent.append((only, copy))
        return copy

    def whole(self, ref, device, group):
        send = self.send.at[self.shared["send", group]]
        recv = self.recv.at[self.shared.get(("recv", group), 0)]
        return pltpu.make_async_remote_copy(
            src_ref=ref,
            dst_ref=ref,
            send_sem=send,
            recv_sem=recv,
            device_id=device,
            device_id_type=MESH,
        )


def kernel(
    nseq, nhead, subs,
    q_in, lat_in, ku_in, vu_in, do_in, pos_in,
    dq_ref, dl_ref, dk_ref, dv_ref,
    q_ref, lat_ref, do_ref, pos_ref, load,
    stage, qd, qall, dall, lat, pos, kt, vt, kuv, ut, sc, dp, mx, sinv, sdel,
    pr, ds, kvg, rp, up, ur, ug, fin, lg, rc, ry, rx, ac, rz, fl, dqt, dqr,
    send, recv,
):
    seq, head = lax.axis_index("seq"), lax.axis_index("head")
    rows = lat_in.shape[1]
    heads = ku_in.shape[1] // D_NOPE
    nq, nk = heads * rows, nseq * rows
    nb = nseq.bit_length() - 1
    hb = heads.bit_length() - 1
    slot_bits = list(range(1, 1 + hb))
    group_bits = list(range(1 + hb, nb))
    groups = 1 << len(group_bits)
    nz = nseq // 2
    scale = 1.0 / math.sqrt(D_QK)
    sems = Sems(send, recv)
    u, w = pick(seq, slot_bits), pick(seq, group_bits)
    x, z = bit(seq, 0), seq // 2
    core, y = bit(head, 0), bit(head, 1)
    active, passive = core == x, core != x

    def on_seq(s):
        return (s, head)

    def on_head(h):
        return (seq, h)

    other = on_head(flip(head, 0))
    across = on_head(flip(head, 1))
    corner = on_head(flip(flip(head, 0), 1))

    barrier = pltpu.get_barrier_semaphore()
    for mask in range(1, nseq):
        pl.semaphore_signal(barrier, inc=1, device_id=on_seq(xor(seq, mask)), device_id_type=MESH)
    for device in (other, across, corner):
        pl.semaphore_signal(barrier, inc=1, device_id=device, device_id_type=MESH)

    def swap(k):
        return (xor(seq, 2 * k) + core - x, head + x - core)

    def greet(k):
        pl.semaphore_signal(barrier, inc=1, device_id=swap(k), device_id_type=MESH)

    for k in range(1, heads):
        greet(k)
    when(passive, lambda: greet(0))

    def at(start, size, step):
        return pl.ds(pl.multiple_of(start * step, step), size)

    mine_k, mine_v = at(u, D_NOPE, D_NOPE), at(u, D_V, D_V)
    loads = [
        pltpu.make_async_copy(src, dst, load.at[k])
        for k, (src, dst) in enumerate((
            (lat_in, lat_ref),
            (q_in, q_ref),
            (do_in, do_ref),
            (pos_in, pos_ref),
            (ku_in.at[:, mine_k], kuv.at[:, :D_NOPE]),
            (vu_in.at[:, mine_v], kuv.at[:, D_NOPE:]),
        ))
    ]
    for copy in loads[:4]:
        copy.start()
    for copy in loads[4:]:
        when(active, copy.start)
    mx[...] = jnp.full(mx.shape, NEG, F32)

    zbits = list(range(nb - 1, 0, -1))
    order = zbits + [0]
    masks = [
        sum(1 << b for b in some)
        for size in range(1, nb + 1)
        for some in itertools.combinations(order, size)
    ]
    zmoves = [m for m in masks if not m & 1]
    by_seq, by_core, by_y, by_both = {}, {}, {}, {}
    sub = D_ALL // nhead

    def quarter(h, s):
        return lat.at[at(h, sub, sub), at(s, rows, rows)]

    def forward(mask):
        piece = quarter(head, xor(seq, mask))
        source = piece if mask else lat_ref.at[at(head, sub, sub)]
        for to in [1] if mask else zmoves + [1]:
            by_seq[mask | to] = sems.copy(
                source, piece, on_seq(xor(seq, to)), group="lat"
            )

    def relay(mask):
        by_seq[mask].wait_recv()
        if not mask & 1:
            forward(mask)
        piece = quarter(head, xor(seq, mask))
        by_y[mask] = sems.copy(piece, piece, across, group="lat")
        by_core[mask] = sems.copy(piece, piece, other, group="lat")

    def relay_y(mask):
        by_y[mask].wait_recv()
        piece = quarter(flip(head, 1), xor(seq, mask))
        by_both[mask] = sems.copy(piece, piece, other, group="lat")

    loads[0].wait()
    pl.semaphore_wait(barrier, nseq + heads + 1 + (core - x) * (core - x))
    forward(0)
    loads[3].wait()
    for mask in range(1, nseq):
        sems.copy(pos_ref, pos.at[seq], on_seq(xor(seq, mask)), group="pos", arrive=True)
    pos_got = sems.whole(pos.at[pl.ds(0, nseq - 1)], other, "pos")
    for copy in loads[1:3]:
        copy.wait()
    for h in range(heads):
        stage[h, :D_QK, :] = q_ref[:, h * D_QK : (h + 1) * D_QK].T
        stage[h, D_QK:, :] = do_ref[:, h * D_V : (h + 1) * D_V].T
    q_got = {}
    for k in range(heads):
        q_got[k] = sems.copy(
            stage.at[pick(xor(seq, 2 * k), slot_bits)],
            qd.at[:, at(u, rows, rows)],
            swap(k),
            None if k else passive,
        )
    for copy in loads[4:]:
        when(active, copy.wait)
    kuv_got = sems.copy(kuv, kuv, other, active)
    lat[:, at(seq, rows, rows)] = lat_ref[...]
    pos[seq] = pos_ref[...]

    @pl.when(active)
    def _():
        qd[:, at(u, rows, rows)] = stage[u]

    def keys_of(s):
        here = at(s, rows, rows)
        both = nn(ut[...], lat[:D_LAT, here]).astype(BF16)
        kt[:D_NOPE, here] = both[:D_NOPE]
        vt[:, here] = both[D_NOPE:]
        kt[D_NOPE:, here] = lat[D_LAT:, here]

    down = lax.broadcasted_iota(jnp.int32, (STRIPE, rows), 0)
    per = rows // STRIPE
    lane = jnp.concatenate([lax.broadcasted_iota(jnp.int32, (1, STRIPE), 1)] * per, axis=1)

    def scores_of(s, k):
        here = at(s, rows, rows)
        keys, vals = kt[:, here], vt[:, here]
        rel = pos[s] - down
        first = pos[xor(seq, 2 * k) + core - x] - lane
        slot = pick(xor(seq, 2 * k), slot_bits)
        for t in range(per):
            part = at(slot * per + t, STRIPE, STRIPE)
            base = first[:, t * STRIPE : (t + 1) * STRIPE]
            base = jnp.concatenate([base] * per, axis=1)
            got = jnp.where(rel <= base, nn(qall[part, :], keys), NEG)
            sc[part, here] = got
            dp[part, here] = nn(dall[part, :], vals)
            top = mx[part, :]
            for c in range(rows // LANE):
                top = jnp.maximum(top, got[:, c * LANE : (c + 1) * LANE])
            mx[part, :] = top

    def scores_pair(p, k):
        here = slice(2 * p * rows, 2 * (p + 1) * rows)
        keys, vals = kt[:, here], vt[:, here]
        rel = jnp.concatenate([pos[2 * p] - down, pos[2 * p + 1] - down], axis=1)
        first = pos[xor(seq, 2 * k) + core - x] - lane
        slot = pick(xor(seq, 2 * k), slot_bits)
        for t in range(per):
            part = at(slot * per + t, STRIPE, STRIPE)
            base = first[:, t * STRIPE : (t + 1) * STRIPE]
            base = jnp.concatenate([base] * (2 * per), axis=1)
            got = jnp.where(rel <= base, nn(qall[part, :], keys), NEG)
            sc[part, here] = got
            dp[part, here] = nn(dall[part, :], vals)
            top = mx[part, :]
            for c in range(2 * rows // LANE):
                top = jnp.maximum(top, got[:, c * LANE : (c + 1) * LANE])
            mx[part, :] = top

    def turn(k):
        if k:
            q_got[k].wait_recv()
        else:
            when(passive, q_got[0].wait_recv)
        here = at(pick(xor(seq, 2 * k), slot_bits), rows, rows)
        qall[here, :] = qd[:D_QK, here].T
        dall[here, :] = qd[D_QK:, here].T

    def block_of(mask):
        by_core[mask].wait_recv()
        by_both[mask].wait_recv()
        keys_of(xor(seq, mask))

    for mask in zmoves + [1]:
        relay(mask)
    when(passive, kuv_got.wait_recv)
    ut[...] = kuv[...].T
    keys_of(seq)
    early = range(heads // 2)
    relay(zmoves[0] | 1)
    turn(0)
    for mask in zmoves[1:]:
        relay(mask | 1)
    pos_got.wait_recv()
    turn(1)
    steps = zmoves + [1] + [mask | 1 for mask in zmoves]
    behind = [0]
    for mask in steps:
        relay_y(mask)
        if len(behind) > 2:
            block = behind.pop(1)
            block_of(block)
            for k in early:
                scores_of(xor(seq, block), k)
        elif behind == [0]:
            for k in early:
                scores_of(seq, k)
        behind.append(mask)
    for block in behind[1:]:
        block_of(block)
        for k in early:
            scores_of(xor(seq, block), k)
    for k in range(heads // 2, heads):
        turn(k)
        for p in range(nz):
            scores_pair(p, k)

    first_sent, sems.sent = sems.sent, []

    def drain(sent):
        for only in (None, active, passive):
            some = [copy for kind, copy in sent if kind is only]

            def act():
                for copy in some:
                    copy.wait_send()

            if some:
                when(only, act)

    factor = scale * LOG2E
    for t in range(nq // STRIPE):
        part = slice(t * STRIPE, (t + 1) * STRIPE)
        top = jnp.max(mx[part, :], axis=1, keepdims=True) * factor

        def sums(k, carry):
            total, weighted = carry
            here = at(k, LANE, LANE)
            e = jnp.exp2(sc[part, here] * factor - top)
            sc[part, here] = e
            return total + e, weighted + e * dp[part, here]

        zero = jnp.zeros((STRIPE, LANE), F32)
        total, weighted = loop(nk // LANE, sums, (zero, zero))
        total = jnp.sum(total, axis=1, keepdims=True)
        weighted = jnp.sum(weighted, axis=1, keepdims=True)
        inv = 1.0 / total
        sinv[part, :] = jnp.broadcast_to(inv, (STRIPE, LANE))
        sdel[part, :] = jnp.broadcast_to(weighted * inv, (STRIPE, LANE))

        def norm(k, carry):
            here = at(k, LANE, LANE)
            prob = sc[part, here] * sinv[part, :]
            sc[part, here] = prob
            pr[part, here] = prob.astype(BF16)
            return carry

        loop(nk // LANE, norm, 0)

    tile = math.gcd(nk, 512)

    def values_grad(k, carry):
        here = at(k, tile, tile)
        kvg[D_NOPE:, here] = nn(qd[D_QK:, :], pr[:, here]).astype(BF16)
        return carry

    loop(nk // tile, values_grad, 0)
    up[0] = nt(lat[:D_LAT, :], kvg[D_NOPE:, :]).astype(BF16)

    share = D_LAT // groups
    piece = share // subs

    summed, moved = {}, {}

    def source(a, i, g):
        return up.at[a, at(g * subs + i, piece, piece)]

    def place(i, s):
        return (
            at(pick(s, group_bits) * subs + i, piece, piece),
            at(pick(s, slot_bits), LANE, LANE),
        )

    def sum_start(a, i):
        for g in range(groups):
            part = at(g * subs + i, piece, piece)
            summed[a, i, g] = sems.copy(up.at[a, part], ur.at[a, part], other, passive)

    def add_up(a, i, g, ref):
        def act():
            kept = source(a, i, g)
            kept[...] = (kept[...].astype(F32) + ref[...].astype(F32)).astype(BF16)

        when(active, act)

    def sum_end(a, i):
        for g in range(groups):
            when(active, summed[a, i, g].wait_recv)
            add_up(a, i, g, ur.at[a, at(g * subs + i, piece, piece)])
        bits, slot = group_bits[::-1], 0
        for k, b in enumerate(bits):
            rest, copies = bits[k + 1 :], []
            for values in itertools.product((0, 1), repeat=len(rest)):
                to, own = flip(seq, b), seq
                for r, value in zip(rest, values):
                    to = to + (1 << r) * (value - bit(to, r))
                    own = own + (1 << r) * (value - bit(own, r))
                copy = sems.copy(
                    source(a, i, pick(to, group_bits)),
                    ug.at[a, i, slot],
                    on_seq(flip(seq, b)),
                    active,
                )
                copies.append((copy, slot, pick(own, group_bits)))
                slot += 1
            for copy, at_slot, g in copies:
                when(active, copy.wait_recv)
                add_up(a, i, g, ug.at[a, i, at_slot])

    def spread(a, i, mask, bits):
        r, c = place(i, xor(seq, mask))
        piece_at = fin.at[a, r, c]
        for b in bits:
            moved[a, i, mask | (1 << b)] = sems.copy(
                piece_at if mask else source(a, i, w),
                piece_at,
                on_seq(flip(seq, b)),
                active,
                "z" if b else "x",
            )

    def spread_z(a, i, mask):
        last = max([k for k, b in enumerate(zbits) if (mask >> b) & 1], default=-1)
        spread(a, i, mask, zbits[last + 1 :])

    def spread_x(a, i, mask):
        spread(a, i, mask, [0])

    def arrive(a, i, mask):
        when(passive if mask & 1 else active, moved[a, i, mask].wait_recv)

    def finish(a, i, mask):
        r, c = place(i, xor(seq, mask))

        def act():
            got = fin[a, r, c] if mask else source(a, i, w)[...]
            (dk_ref if a else dv_ref)[r, c] = got.astype(F32)

        when(passive if mask & 1 else active, act)

    for i in range(subs):
        sum_start(0, i)

    for t in range(nq // STRIPE):
        part = slice(t * STRIPE, (t + 1) * STRIPE)

        def scored(k, carry):
            here = at(k, LANE, LANE)
            ds[part, here] = (
                sc[part, here] * (dp[part, here] - sdel[part, :]) * scale
            ).astype(BF16)
            return carry

        loop(nk // LANE, scored, 0)

    for i in range(subs):
        sum_end(0, i)
        spread_z(0, i, 0)
        spread_x(0, i, 0)
    dqt[...] = nt(kt[...], ds[...]).astype(BF16)
    dq_in = [
        sems.copy(
            dqt.at[:, at(pick(xor(seq, 2 * k), slot_bits), rows, rows)],
            dqr.at[u],
            swap(k),
            None if k else passive,
        )
        for k in range(heads)
    ]

    @pl.when(active)
    def _():
        dqr[u] = dqt[:, at(u, rows, rows)]

    def keys_grad(k, carry):
        here = at(k, tile, tile)
        got = nn(qd[:D_QK, :], ds[:, here]).astype(BF16)
        kvg[:D_NOPE, here] = got[:D_NOPE]
        rp[:, here] = got[D_NOPE:]
        return carry

    loop(nk // tile, keys_grad, 0)

    zmasks = list(range(1, nz))[::-1] + [0]
    to_core, to_y, to_x, to_z = {}, {}, {}, {}
    mine, others = y * 2 + core, (1 - y) * 2 + core

    def fold(k):
        here = at(xor(z, k), 2 * rows, 2 * rows)
        got = nn(kuv[...], kvg[:, here]).astype(BF16)
        got = jnp.concatenate([got, rp[:, here]], axis=0)
        for h in range(nhead):
            lg[h, k] = got[h * sub : (h + 1) * sub]

    def share_fold(k):
        to_core[k] = [
            sems.copy(lg.at[t * 2 + 1 - core, k], rc.at[j, k], other, group="wide")
            for j, t in ((0, 1 - y), (1, y))
        ]

    def add_core(k):
        to_core[k][0].wait_recv()
        lg[others, k] = (lg[others, k].astype(F32) + rc[0, k].astype(F32)).astype(BF16)
        to_y[k] = sems.copy(lg.at[others, k], ry.at[k], across, group="wide")
        to_core[k][1].wait_recv()
        lg[mine, k] = (lg[mine, k].astype(F32) + rc[1, k].astype(F32)).astype(BF16)

    def add_y(k):
        to_y[k].wait_recv()
        lg[mine, k] = (lg[mine, k].astype(F32) + ry[k].astype(F32)).astype(BF16)
        to_x[k] = sems.copy(
            lg.at[mine, k, :, at(1 - x, rows, rows)],
            rx.at[k],
            on_seq(flip(seq, 0)),
            group="narrow",
        )

    def add_x(k):
        to_x[k].wait_recv()
        kept = lg[mine, k, :, at(x, rows, rows)].astype(F32) + rx[k].astype(F32)
        ac[k] = kept.astype(BF16)
        if k:
            to_z[k] = sems.copy(ac.at[k], rz.at[k], on_seq(xor(seq, 2 * k)), group="narrow")

    chunks = [(a, i) for a in range(2) for i in range(subs)]
    values, keys = chunks[:subs], chunks[subs:]
    near_z = [m for m in zmoves if m.bit_count() == 1]
    far_z = [m for m in zmoves if m.bit_count() > 1]

    for k in zmasks:
        fold(k)
    for k in zmasks:
        share_fold(k)
    up[1] = nt(lat[:D_LAT, :], kvg[:D_NOPE, :]).astype(BF16)
    for i in range(subs):
        sum_start(1, i)
    for k in zmasks:
        add_core(k)
    for a, i in keys:
        sum_end(a, i)
        spread_z(a, i, 0)
        spread_x(a, i, 0)
    for chunk in chunks:
        finish(*chunk, 0)

    held = []

    def along_z(some, mask, hold=False):
        for chunk in some:
            arrive(*chunk, mask)
            spread_z(*chunk, mask)
            if hold:
                held.append((*chunk, mask))
            else:
                spread_x(*chunk, mask)
            finish(*chunk, mask)

    for mask in near_z[1:][::-1]:
        along_z(values, mask)
    drain(first_sent)
    sems.whole(lat.at[:, pl.ds(0, (nseq - 1) * rows)], other, "lat").wait_send()
    pos_got.wait_send()
    for k in zmasks[:-1]:
        add_y(k)
    for mask in near_z[1:][::-1]:
        along_z(keys, mask)
    for k in zmasks[:-3]:
        add_x(k)
    along_z(values, near_z[0])
    for k in zmasks[-1:]:
        add_y(k)
    for k in zmasks[-3:-2]:
        add_x(k)
    along_z(keys, near_z[0], True)
    for k in zmasks[-2:-1]:
        add_x(k)
    for move in held:
        spread_x(*move)
    last_sent, sems.sent = sems.sent, []
    for mask in far_z:
        along_z(chunks, mask)
    add_x(0)
    total = ac[0].astype(F32)
    for k in zmasks[:-1]:
        to_z[k].wait_recv()
        total = total + rz[k].astype(F32)
    fl[head] = total.astype(BF16)
    first = sems.copy(fl.at[head], fl.at[head], across, group="narrow")
    third = sems.copy(fl.at[head], fl.at[head], corner, group="narrow")
    second = sems.copy(fl.at[head], fl.at[head], other, group="narrow")
    drain(last_sent)
    when(active, sems.whole(fin.at[:, : D_LAT * (nz - 1) // nz], other, "z").wait_send)
    sems.whole(lg.at[: nhead - 1], other, "wide").wait_send()
    for copy in dq_in[1:]:
        copy.wait_recv()
    when(passive, dq_in[0].wait_recv)
    for h in range(heads):
        dq_ref[:, h * D_QK : (h + 1) * D_QK] = dqr[h].T
    first.wait_recv()
    for mask in [0] + zmoves:
        for chunk in chunks:
            arrive(*chunk, mask | 1)
            finish(*chunk, mask | 1)
    second.wait_recv()
    third.wait_recv()
    for h in range(nhead):
        dl_ref[h * sub : (h + 1) * sub, :] = fl[h].astype(F32)
    assert (sems.sends, sems.recvs) == (send.shape[0], recv.shape[0])
    drain(sems.sent)
    when(active, sems.whole(fin, other, "x").wait_send)
    sems.whole(lat.at[: 2 * sub, pl.ds(0, (nz + 1) * rows)], other, "narrow").wait_send()


def store(*refs):
    sems = refs[8]
    copies = [pltpu.make_async_copy(refs[k], refs[4 + k], sems.at[k]) for k in range(4)]
    for copy in copies:
        copy.start()
    for copy in copies:
        copy.wait()


def make_shards(nseq, nhead):
    def shards(queries, latents, key_up, value_up, out_grad, positions):
        rows, heads = latents.shape[0], key_up.shape[1] // D_NOPE
        nq, nk = heads * rows, nseq * rows
        nz, groups = nseq // 2, nseq // (2 * heads)
        subs = 2
        share = D_LAT // groups
        sub = D_ALL // nhead
        cols = key_up.shape[1]
        sums = 2 * subs * (2 * groups - 1)
        sends = 2 * heads + 1 + sums + 6
        copies = (nseq - 1) * 4 + 1 + 2 * heads + 1
        copies += sums + 2 * subs * (nseq - 1) + 5 * nz + 2
        vmem = pl.BlockSpec(memory_space=pltpu.VMEM)
        body = lambda *refs: kernel(nseq, nhead, subs, *refs)
        moved = [
            (queries.shape, BF16),
            ((D_ALL, rows), BF16),
            (out_grad.shape, BF16),
            ((1, rows), jnp.int32),
        ]
        scratch = [
            ((heads, D_QK + D_V, rows), BF16),
            ((D_QK + D_V, nq), BF16),
            ((nq, D_QK), BF16),
            ((nq, D_V), BF16),
            ((D_ALL, nk), BF16),
            ((nseq, 1, rows), jnp.int32),
            ((D_QK, nk), BF16),
            ((D_V, nk), BF16),
            ((D_LAT, D_NOPE + D_V), BF16),
            ((D_NOPE + D_V, D_LAT), BF16),
            ((nq, nk), F32),
            ((nq, nk), F32),
            ((nq, LANE), F32),
            ((nq, LANE), F32),
            ((nq, LANE), F32),
            ((nq, nk), BF16),
            ((nq, nk), BF16),
            ((D_NOPE + D_V, nk), BF16),
            ((D_ROPE, nk), BF16),
            ((2, D_LAT, LANE), BF16),
            ((2, D_LAT, LANE), BF16),
            ((2, subs, max(groups - 1, 1), share // subs, LANE), BF16),
            ((2, D_LAT, cols), BF16),
            ((nhead, nz, sub, 2 * rows), BF16),
            ((nhead // 2, nz, sub, 2 * rows), BF16),
            ((nz, sub, 2 * rows), BF16),
            ((nz, sub, rows), BF16),
            ((nz, sub, rows), BF16),
            ((nz, sub, rows), BF16),
            ((nhead, sub, rows), BF16),
            ((D_QK, nq), BF16),
            ((heads, D_QK, rows), BF16),
        ]
        limit = 8 * 1024 * 1024
        for shape, dtype in moved + scratch:
            padded = (-(-shape[-1] // LANE) * LANE) * (-(-shape[-2] // 16) * 16)
            limit += math.prod(shape[:-2]) * padded * jnp.dtype(dtype).itemsize
        dq, dl, dk, dv = pl.pallas_call(
            body,
            out_shape=(
                jax.ShapeDtypeStruct(queries.shape, BF16),
                jax.ShapeDtypeStruct((D_ALL, rows), F32),
                jax.ShapeDtypeStruct(key_up.shape, F32),
                jax.ShapeDtypeStruct(value_up.shape, F32),
            ),
            in_specs=[pl.BlockSpec(memory_space=pltpu.HBM)] * 6,
            out_specs=(vmem,) * 4,
            scratch_shapes=[pltpu.VMEM(shape, dtype) for shape, dtype in moved]
            + [pltpu.SemaphoreType.DMA((6,))]
            + [pltpu.VMEM(shape, dtype) for shape, dtype in scratch]
            + [pltpu.SemaphoreType.DMA((sends,)), pltpu.SemaphoreType.DMA((copies,))],
            compiler_params=pltpu.CompilerParams(
                collective_id=0, has_side_effects=True, vmem_limit_bytes=min(limit, 60 * 1024 * 1024)
            ),
        )(*[
            pltpu.with_memory_space_constraint(a, pltpu.HBM)
            for a in (queries, latents.T, key_up, value_up, out_grad, positions[None, :])
        ])
        done = (dq, dl, dk, dv)
        dq, dl, dk, dv = pl.pallas_call(
            store,
            out_shape=[jax.ShapeDtypeStruct(a.shape, a.dtype) for a in done],
            in_specs=[vmem] * 4,
            out_specs=[pl.BlockSpec(memory_space=pltpu.HBM)] * 4,
            scratch_shapes=[pltpu.SemaphoreType.DMA((4,))],
            compiler_params=pltpu.CompilerParams(vmem_limit_bytes=1024 * 1024),
        )(*done)
        return dq, dl.T, dk, dv

    return shards


def solution(mesh):
    in_specs = (
        P("seq", "head"),
        P("seq", None),
        P(None, "head"),
        P(None, "head"),
        P("seq", "head"),
        P("seq"),
    )
    out_specs = (P("seq", "head"), P("seq", None), P(None, "head"), P(None, "head"))
    shards = make_shards(mesh.shape["seq"], mesh.shape["head"])
    return jax.shard_map(shards, mesh=mesh, in_specs=in_specs, out_specs=out_specs, check_vma=False)
```
